1024 devices in a mesh: dp: 16 (over x, core), seq: 8 (over z), tensor: 8 (over y).
Axes of the slice: x: 8, y: 8, z: 8, core: 2. Of those that a mesh axis runs over, the one named last changes fastest.
Arguments:
- vit_out: bfloat16 [32768, 3200], P(('dp', 'seq')), may hold values from -6 to 6
- ln_gain: float32 [3200], replicated, may hold values from 0.1 to 1.9
- ln_bias: float32 [3200], replicated, may hold values from -3 to 3
- proj_weight: bfloat16 [3200, 8, 1024], P(None, None, 'tensor'), may hold values from -0.109375 to 0.109375
- proj_bias: float32 [8, 1024], P(None, 'tensor'), may hold values from -3 to 3
- text_embed: bfloat16 [65536, 8192], P('dp', ('seq', 'tensor')), may hold values from -6 to 6
- norm_gain: float32 [8192], P(('seq', 'tensor')), may hold values from 0.1 to 1.9
- tile_dest: int32 [256, 1], replicated, may hold values from 0 to 15; in each aligned block of 16 rows (0 to 15, 16 to 31, ...) at most 2 rows name the same one
- tile_place: int32 [16, 32], replicated, may hold values from 0 to 31, each once within a row
Outputs:
- normed: bfloat16 [65536, 8192], P('dp', ('seq', 'tensor'))
The draws below stay inside these ranges and needn't reach their ends.
Inputs may be any that keep to these rules, and one draw needn't show every extreme that they name: `tile_dest`: in each aligned block of 16 rows (one encoder group's tiles) no replica is named more than 2 times, a bound that some block reaches. `tile_place`: each row is a permutation of 0 to 31.
All inputs are finite; a program needn't handle non-finite values.
Results may differ from the reference program's by a relative error of at most 0.0048.
Values may be sent and summed in bfloat16 or wider, within the bound.
A program may use at most 64 MiB of HBM per device.

```python
import math
import jax
import jax.numpy as jnp
import numpy as np
from jax import lax

VD = 3200
D = 8192
TILE = 128
SEQS = 4
SEQ_LEN = 1024
GROUP_TILES = 16
CAP = 2
POSITIONS = 32
N_DP = 16
N_SEQ = 8


def block_levels(key, extent, split, smallest, top_value):
    def one(dim, shards_of):
        steps = jax.random.uniform(jax.random.fold_in(jax.random.fold_in(key, 6), dim), (shards_of,), jnp.float32, smallest / len(split), top_value / len(split))
        return jnp.repeat(jnp.exp(steps), extent[dim] // shards_of).reshape((-1,) + (1,) * (len(extent) - dim - 1))

    loudness = one(*split[0])
    for cut in split[1:]:
        loudness = loudness * one(*cut)
    return loudness


def assign_block(rng, own, number, rows, count, top, most, slope):
    order = jax.random.permutation(rng, count)
    packed, common = shares(count, rows * top, most, slope, True), shares(count, rows * top, most, slope, False)
    places = jnp.arange(count)

    def named(lengths, turn):
        used = int((lengths > 0).sum())
        fixed = max(1, used // 4)
        passed = fixed + (places - fixed + turn * (used - fixed)) % max(1, count - fixed)
        return jnp.zeros((count,), jnp.int32).at[order[jnp.where(places < fixed, places, passed)]].set(jnp.asarray(lengths, jnp.int32))

    lengths = jnp.where(number % 4 == 0, named(packed, number // 4), named(common, number - number // 4 - 1))
    mixed = jax.random.permutation(jax.random.fold_in(own, 3), count)
    source_of, taker = mixed[0:count // 2 * 2:2], mixed[1:count // 2 * 2:2]
    room = jnp.minimum(lengths[source_of] - 1, most - lengths[taker]) // 2
    room = jnp.where((source_of == order[0]) | (taker == order[0]) | (lengths[taker] == 0), 0, jnp.maximum(room, 0))
    passed = jax.random.randint(jax.random.fold_in(own, 4), (count // 2,), 0, 1 << 20) % (room + 1)
    lengths = lengths.at[source_of].add(-passed).at[taker].add(passed)
    items = jnp.searchsorted(jnp.cumsum(lengths), jnp.arange(rows * top), side="right").astype(jnp.int32)
    grid = items.reshape(top, rows).T
    grid = grid[jax.random.permutation(jax.random.fold_in(own, 1), rows)]
    turn = jax.random.randint(jax.random.fold_in(own, 2), (rows, 1), 0, top)
    return jnp.take_along_axis(grid, (jnp.arange(top)[None, :] + turn) % top, axis=1)


def shares(amount, total, most, lean, full):
    portions = [(1 << 20) // math.isqrt(rank ** lean) + 1 for rank in range(1, amount + 1)]
    largest = most if full else min(most, max(-(-total // amount), total * portions[0] // sum(portions)))
    least = 1 if total - largest >= amount - 1 else 0
    counts, spare = [largest] + [least] * (amount - 1), total - largest - least * (amount - 1)
    while spare > 0:
        candidates = [i for i in range(1, amount) if counts[i] < largest] or [i for i in range(1, amount) if counts[i] < most]
        pool, remaining = sum([portions[i] for i in candidates]), spare
        for i in candidates:
            extra = min(most - counts[i], max(1, remaining * portions[i] // pool), spare)
            counts[i] = counts[i] + extra
            spare = spare - extra
    return np.array(counts)


def bell_draw(key, extent, deviation, reach, shards=(), kind=jnp.bfloat16):
    gain = block_levels(key, extent, shards, -0.22, 0.18) if shards else 1.0
    array = jax.random.normal(key, extent, jnp.float32) * deviation * gain
    return jnp.minimum(jnp.maximum(array, -reach), reach).astype(kind)


def setup_inputs(seed: int = 0) -> dict:
    arg_keys = jax.random.split(jax.random.key(seed), 10)
    vit_out = bell_draw(arg_keys[0], (N_DP * GROUP_TILES * TILE, VD), 1.0, 6.0, ((0, 128),))
    ln_gain = jnp.clip(1.0 + 0.18 * jax.random.normal(arg_keys[1], (VD,), jnp.float32), 0.1, 1.9)
    ln_bias = bell_draw(arg_keys[2], (VD,), 0.5, 3.0, (), jnp.float32)
    proj_weight = bell_draw(arg_keys[3], (VD, N_SEQ, D // N_SEQ), VD ** -0.5, 0.109375, ((2, 8),))
    proj_bias = bell_draw(arg_keys[4], (N_SEQ, D // N_SEQ), 0.5, 3.0, ((1, 8),), jnp.float32)
    text_embed = bell_draw(arg_keys[5], (N_DP * SEQS * SEQ_LEN, D), 1.0, 6.0, ((0, 16), (1, 64)))
    norm_gain = jnp.clip(1.0 + 0.18 * jax.random.normal(arg_keys[6], (D,), jnp.float32), 0.1, 1.9)
    tile_dest_keys = jax.random.split(jax.random.fold_in(arg_keys[7], 1), (N_DP * GROUP_TILES) // GROUP_TILES)
    tile_dest_turns = jax.random.permutation(jax.random.fold_in(arg_keys[7], 3), (N_DP * GROUP_TILES) // GROUP_TILES)
    tile_dest = jax.vmap(lambda own, number: assign_block(jax.random.fold_in(arg_keys[7], 2), own, number, GROUP_TILES, N_DP, 1, CAP, 2))(tile_dest_keys, tile_dest_turns).reshape((N_DP * GROUP_TILES, 1))
    tile_place = jax.vmap(lambda own: jax.random.permutation(own, POSITIONS))(jax.random.split(arg_keys[8], N_DP)).reshape((N_DP, POSITIONS)).astype(jnp.int32)
    return {"vit_out": vit_out, "ln_gain": ln_gain, "ln_bias": ln_bias, "proj_weight": proj_weight, "proj_bias": proj_bias, "text_embed": text_embed, "norm_gain": norm_gain, "tile_dest": tile_dest, "tile_place": tile_place}


def layer_norm(rows, ln_gain, ln_bias):
    values = rows.astype(jnp.float32)
    center = values - lax.optimization_barrier(jnp.mean(values, axis=-1, keepdims=True))
    spread = lax.optimization_barrier(jnp.mean(center * center, axis=-1, keepdims=True))
    return (center * lax.rsqrt(spread + 1e-06) * ln_gain + ln_bias).astype(jnp.bfloat16)

def arrival_ranks(destination, replicas):
    onehot = (destination[:, None] == jnp.arange(replicas, dtype=jnp.int32)[None, :]).astype(jnp.int32)
    before = jnp.cumsum(onehot, axis=0) - onehot
    return lax.optimization_barrier(jnp.sum(before * onehot, axis=1))

def reference(vit_out, ln_gain, ln_bias, proj_weight, proj_bias, text_embed, norm_gain, tile_dest, tile_place):
    weights = proj_weight.reshape(VD, D)
    bias_flat = proj_bias.reshape(D)

    def project(rows):
        normed_in = layer_norm(rows, ln_gain, ln_bias)
        hidden = jnp.dot(normed_in, weights, preferred_element_type=jnp.float32) + bias_flat
        return hidden.astype(jnp.bfloat16)
    projected = lax.map(project, vit_out.reshape(N_DP, GROUP_TILES * TILE, VD))
    tiles = projected.reshape(N_DP * GROUP_TILES, TILE, D)
    total_tiles = N_DP * GROUP_TILES
    destination = tile_dest[:, 0].astype(jnp.int32)
    ranks = arrival_ranks(destination, N_DP)
    slots = tile_place[destination, ranks].astype(jnp.int32)
    target = destination * POSITIONS + slots
    source_tile = jnp.full((N_DP * POSITIONS,), -1, jnp.int32).at[target].set(jnp.arange(total_tiles, dtype=jnp.int32))
    source_tile = source_tile.reshape(N_DP, POSITIONS)
    text_tiles = text_embed.reshape(N_DP, POSITIONS, TILE, D)

    def assemble(items):
        sources, text_part = items
        picked = tiles[jnp.clip(sources, 0, total_tiles - 1)]
        assembled = jnp.where((sources >= 0)[:, None, None], picked, text_part).reshape(POSITIONS * TILE, D)
        values = assembled.astype(jnp.float32)
        mean_square = lax.optimization_barrier(jnp.sum(values * values, axis=-1)) / D
        return (values * lax.rsqrt(mean_square + 1e-05)[:, None] * norm_gain).astype(jnp.bfloat16)
    result = lax.map(assemble, (source_tile, text_tiles))
    return result.reshape(N_DP * POSITIONS * TILE, D)
```

```python
import functools

import jax
import jax.numpy as jnp
from jax import lax
from jax.experimental import pallas as pl
from jax.experimental.pallas import tpu as pltpu
from jax.sharding import PartitionSpec as P

D = 8192
TILE = 128
CAP = 2
CHUNKS = 4
MESH = pl.DeviceIdType.MESH


def layer_norm(rows, ln_gain, ln_bias):
    values = rows.astype(jnp.float32)
    center = values - jnp.mean(values, axis=-1, keepdims=True)
    spread = jnp.mean(center * center, axis=-1, keepdims=True)
    return (center * lax.rsqrt(spread + 1e-06) * ln_gain + ln_bias).astype(jnp.bfloat16)


def spiral(n):
    order = [n // 2]
    for d in range(n // 2 - 1, 0, -1):
        order += [d, n - d]
    return order


def lane_sums(squares):
    ones = jnp.ones((8, squares.shape[1]), jnp.bfloat16)
    dims = (((1,), (1,)), ((), ()))
    high = squares.astype(jnp.bfloat16)
    low = (squares - high.astype(jnp.float32)).astype(jnp.bfloat16)
    return lax.dot_general(
        ones, high, dims, preferred_element_type=jnp.float32
    ) + lax.dot_general(ones, low, dims, preferred_element_type=jnp.float32)


def exchange_kernel(
    sizes,
    proj,
    text_hbm,
    gain,
    dest,
    place,
    out_hbm,
    text,
    out,
    scales,
    part,
    ybuf,
    zbuf,
    isums,
    tsums,
    xsend,
    xsums,
    table,
    kinv,
    starts,
    *rest,
):
    replicas, owners, tensors, positions = sizes
    rows = TILE // CHUNKS
    group_tiles = 2 * owners
    tiles, slots, inc = rest[:CHUNKS], rest[CHUNKS : 2 * CHUNKS], rest[2 * CHUNKS : 3 * CHUNKS]
    (zs, zr, xs, xr, ys, yr, zss, zsr, xss, xsr, tsem, osem) = rest[3 * CHUNKS :]
    me_dp, me_s, me_t = lax.axis_index("dp"), lax.axis_index("seq"), lax.axis_index("tensor")

    def peer(me, k, n):
        return lax.rem(me + k, n)

    barrier = pltpu.get_barrier_semaphore()
    axes = (("dp", me_dp, replicas), ("seq", me_s, owners), ("tensor", me_t, tensors))
    for name, me, n in axes:
        for k in spiral(n):
            pl.semaphore_signal(
                barrier, inc=1, device_id={name: peer(me, k, n)}, device_id_type=MESH
            )
    load_text = pltpu.make_async_copy(text_hbm, text, tsem)
    load_text.start()
    pl.semaphore_wait(barrier, replicas + owners + tensors - 3)

    zcopies = []
    for h in range(CHUNKS):
        for k in spiral(owners):
            to = peer(me_s, k, owners)
            zcopies.append(
                pltpu.make_async_remote_copy(
                    src_ref=proj.at[to, :, pl.ds(h * rows, rows), :],
                    dst_ref=tiles[h].at[pl.ds(2 * me_s, 2)],
                    send_sem=zs.at[h, k],
                    recv_sem=zr.at[h, k],
                    device_id={"seq": to},
                    device_id_type=MESH,
                )
            )
            zcopies[-1].start()
    for h in range(CHUNKS):
        tiles[h][pl.ds(2 * me_s, 2)] = proj[me_s, :, h * rows : (h + 1) * rows, :]

    load_text.wait()
    sub = lax.broadcasted_iota(jnp.int32, (8, TILE), 0)

    def sum_text(b, carry):
        values = text[pl.ds(8 * b, 8)].astype(jnp.float32).reshape(8 * TILE, TILE)
        sums = lane_sums(values * values)
        total = jnp.zeros((8, TILE), jnp.float32)
        for i in range(8):
            total = jnp.where(sub == i, sums[:, i * TILE : (i + 1) * TILE], total)
        part[pl.ds(pl.multiple_of(8 * b, 8), 8), :] = total
        return carry

    lax.fori_loop(0, positions // 8, sum_text, 0)
    squares = jnp.zeros((2 * TILE, TILE), jnp.float32)
    for s in range(owners):
        values = proj[s].astype(jnp.float32).reshape(2 * TILE, TILE)
        squares = squares + values * values
    sums = lane_sums(squares)
    part[positions : positions + 8, :] = jnp.where(sub == 0, sums[:, :TILE], sums[:, TILE:])

    ycopies = []
    for k in spiral(tensors):
        to = peer(me_t, k, tensors)
        ycopies.append(
            pltpu.make_async_remote_copy(
                src_ref=part,
                dst_ref=ybuf.at[me_t],
                send_sem=ys.at[k],
                recv_sem=yr.at[k],
                device_id={"tensor": to},
                device_id_type=MESH,
            )
        )
        ycopies[-1].start()

    for r in range(replicas):
        first = jnp.int32(group_tiles - 1)
        last = jnp.int32(0)
        for j in range(group_tiles):
            hit = dest[me_dp * group_tiles + j] == r
            last = jnp.where(hit, j, last)
            hit_back = dest[me_dp * group_tiles + group_tiles - 1 - j] == r
            first = jnp.where(hit_back, group_tiles - 1 - j, first)
        table[2 * r] = first
        table[2 * r + 1] = last

    def count(g, total):
        starts[g] = total
        for j in range(group_tiles):
            total = total + jnp.where(dest[g * group_tiles + j] == me_dp, 1, 0)
        return total

    starts[replicas] = lax.fori_loop(0, replicas, count, jnp.int32(0))

    def invert(p, carry):
        order = jnp.int32(0)
        for k in range(positions):
            order = jnp.where(place[me_dp, k] == p, k, order)
        slot = jnp.int32(-1)
        for g in range(replicas):
            here = (order >= starts[g]) & (order < starts[g + 1])
            slot = jnp.where(here, 2 * g + order - starts[g], slot)
        kinv[p] = slot
        return carry

    lax.fori_loop(0, positions, invert, 0)

    xcopies = []

    def send_chunk(h):
        for k in spiral(owners):
            zcopies[h * (owners - 1) + spiral(owners).index(k)].wait_recv()
        for k in spiral(replicas) + [0]:
            r = peer(me_dp, k, replicas)
            for c in range(CAP):
                slots[h][2 * r + c] = tiles[h][table[2 * r + c]]
        for k in spiral(replicas):
            to = peer(me_dp, k, replicas)
            xcopies.append(
                pltpu.make_async_remote_copy(
                    src_ref=slots[h].at[pl.ds(2 * to, 2)],
                    dst_ref=inc[h].at[pl.ds(2 * me_dp, 2)],
                    send_sem=xs.at[h, k],
                    recv_sem=xr.at[h, k],
                    device_id={"dp": to},
                    device_id_type=MESH,
                )
            )
            xcopies[-1].start()
        inc[h][pl.ds(2 * me_dp, 2)] = slots[h][pl.ds(2 * me_dp, 2)]

    send_chunk(0)

    for copy in ycopies:
        copy.wait_recv()
    ybuf[me_t] = part[...]
    total = ybuf[0]
    for t in range(1, tensors):
        total = total + ybuf[t]
    zbuf[me_s] = total
    zscopies = []
    for k in spiral(owners):
        to = peer(me_s, k, owners)
        zscopies.append(
            pltpu.make_async_remote_copy(
                src_ref=zbuf.at[me_s],
                dst_ref=zbuf.at[me_s],
                send_sem=zss.at[k],
                recv_sem=zsr.at[k],
                device_id={"seq": to},
                device_id_type=MESH,
            )
        )
        zscopies[-1].start()

    for h in range(1, CHUNKS):
        send_chunk(h)

    for copy in zscopies:
        copy.wait_recv()
    text_total = zbuf[0, :positions]
    for s in range(1, owners):
        text_total = text_total + zbuf[s, :positions]
    tsums[...] = text_total
    for s in range(owners):
        isums[2 * s : 2 * s + 2, :] = zbuf[s, positions : positions + 2]
    for r in range(replicas):
        for c in range(CAP):
            xsend[r, c : c + 1, :] = isums[pl.ds(table[2 * r + c], 1), :]
    xscopies = []
    for k in spiral(replicas):
        to = peer(me_dp, k, replicas)
        xscopies.append(
            pltpu.make_async_remote_copy(
                src_ref=xsend.at[to],
                dst_ref=xsums.at[me_dp],
                send_sem=xss.at[k],
                recv_sem=xsr.at[k],
                device_id={"dp": to},
                device_id_type=MESH,
            )
        )
        xscopies[-1].start()
    xsums[me_dp] = xsend[me_dp]
    for copy in xscopies:
        copy.wait_recv()

    def scale_rows(p, carry):
        slot = kinv[p]
        safe = jnp.maximum(slot, 0)
        image = xsums[safe // 2, pl.ds(lax.rem(safe, 2), 1), :]
        total = jnp.where(slot >= 0, image, tsums[pl.ds(p, 1), :])
        scale = lax.rsqrt(total / D + 1e-05)
        scales[p] = jnp.transpose(jnp.broadcast_to(scale, (TILE, TILE)))
        return carry

    lax.fori_loop(0, positions, scale_rows, 0)

    stores = []
    for h in range(CHUNKS):
        for i in range(replicas - 1):
            xcopies[h * (replicas - 1) + i].wait_recv()

        def finish(p, carry, h=h):
            slot = kinv[p]
            picked = inc[h][jnp.maximum(slot, 0)]
            here = pl.ds(h * rows, rows)
            chosen = jnp.where(slot >= 0, picked, text[p, here, :]).astype(jnp.float32)
            out[p, here, :] = (chosen * scales[p, here, :] * gain[...]).astype(jnp.bfloat16)
            return carry

        lax.fori_loop(0, positions, finish, 0)
        here = pl.ds(h * rows, rows)
        stores.append(
            pltpu.make_async_copy(out.at[:, here, :], out_hbm.at[:, here, :], osem.at[h])
        )
        stores[-1].start()

    for copy in zcopies + ycopies + zscopies + xcopies + xscopies:
        copy.wait_send()
    for copy in stores:
        copy.wait()


def local(
    vit_out, ln_gain, ln_bias, proj_weight, proj_bias, text_embed, norm_gain, tile_dest, tile_place
):
    replicas, owners, tensors = (lax.axis_size(a) for a in ("dp", "seq", "tensor"))
    local_rows = vit_out.shape[0]
    block = proj_weight.shape[2]
    positions = tile_place.shape[1]
    rows = TILE // CHUNKS
    normed_in = layer_norm(vit_out, ln_gain, ln_bias)
    weights = proj_weight.reshape(vit_out.shape[1], owners * block)
    hidden = jnp.dot(normed_in, weights, preferred_element_type=jnp.float32) + proj_bias.reshape(-1)
    projected = hidden.astype(jnp.bfloat16).reshape(2, TILE, owners, block)
    projected = jnp.transpose(projected, (2, 0, 1, 3))
    text = text_embed.reshape(positions, TILE, block)

    vmem, smem = pl.BlockSpec(memory_space=pltpu.VMEM), pl.BlockSpec(memory_space=pltpu.SMEM)
    hbm = pl.BlockSpec(memory_space=pl.ANY)
    bf16, f32, i32 = jnp.bfloat16, jnp.float32, jnp.int32
    dma = pltpu.SemaphoreType.DMA
    out = pl.pallas_call(
        functools.partial(exchange_kernel, (replicas, owners, tensors, positions)),
        out_shape=jax.ShapeDtypeStruct(text.shape, bf16),
        in_specs=[vmem, hbm, vmem, smem, smem],
        out_specs=hbm,
        scratch_shapes=[
            pltpu.VMEM(text.shape, bf16),
            pltpu.VMEM(text.shape, bf16),
            pltpu.VMEM(text.shape, f32),
            pltpu.VMEM((positions + 8, TILE), f32),
            pltpu.VMEM((tensors, positions + 8, TILE), f32),
            pltpu.VMEM((owners, positions + 8, TILE), f32),
            pltpu.VMEM((2 * owners, TILE), f32),
            pltpu.VMEM((positions, TILE), f32),
            pltpu.VMEM((replicas, 8, TILE), f32),
            pltpu.VMEM((replicas, 8, TILE), f32),
            pltpu.SMEM((CAP * replicas,), i32),
            pltpu.SMEM((positions,), i32),
            pltpu.SMEM((replicas + 1,), i32),
        ]
        + [pltpu.VMEM((2 * owners, rows, block), bf16)] * CHUNKS
        + [pltpu.VMEM((CAP * replicas, rows, block), bf16)] * CHUNKS
        + [pltpu.VMEM((CAP * replicas, rows, block), bf16)] * CHUNKS
        + [dma((CHUNKS, owners))] * 2
        + [dma((CHUNKS, replicas))] * 2
        + [dma((tensors,))] * 2
        + [dma((owners,))] * 2
        + [dma((replicas,))] * 2
        + [dma, dma((CHUNKS,))],
        compiler_params=pltpu.CompilerParams(
            collective_id=0, has_side_effects=True, vmem_limit_bytes=32 * 1024 * 1024
        ),
    )(projected, text, norm_gain.reshape(1, block), tile_dest.reshape(-1), tile_place)
    return out.reshape(text_embed.shape)


def solution(mesh):
    placed = (
        P(("dp", "seq"), None),
        P(),
        P(),
        P(None, None, "tensor"),
        P(None, "tensor"),
        P("dp", ("seq", "tensor")),
        P(("seq", "tensor")),
        P(),
        P(),
    )
    return jax.shard_map(
        local, mesh=mesh, in_specs=placed, out_specs=P("dp", ("seq", "tensor")), check_vma=False
    )
```

```python
import functools

import jax
import jax.numpy as jnp
from jax import lax
from jax.experimental import pallas as pl
from jax.experimental.pallas import tpu as pltpu
from jax.sharding import PartitionSpec as P

D = 8192
TILE = 128
CAP = 2
SPANS = (16, 16, 32, 32, 32)
CHUNKS = len(SPANS)
DEPTH = 640
LIMIT = 56
PASSES = ((0,), (1,), (2,), (3, 4))
EARLY = 3
UNROLL = 4
MESH = pl.DeviceIdType.MESH


def spiral(n):
    order = [n // 2]
    for d in range(n // 2 - 1, 0, -1):
        order += [d, n - d]
    return order


def wait_for(ref, sem):
    pltpu.make_async_copy(ref, ref, sem).wait()


def lane_sums(squares):
    ones = jnp.ones((8, squares.shape[1]), jnp.bfloat16)
    dims = (((1,), (1,)), ((), ()))
    high = squares.astype(jnp.bfloat16)
    low = (squares - high.astype(jnp.float32)).astype(jnp.bfloat16)
    return lax.dot_general(
        ones, high, dims, preferred_element_type=jnp.float32
    ) + lax.dot_general(ones, low, dims, preferred_element_type=jnp.float32)


def exchange_kernel(
    sizes,
    vit_hbm,
    weight_hbm,
    ln_gain_hbm,
    ln_bias_hbm,
    bias_hbm,
    text_hbm,
    gain_hbm,
    dest_hbm,
    place_hbm,
    out_hbm,
    out,
    ln_gain,
    ln_bias,
    bias,
    gain,
    dest,
    place,
    lgain,
    lbias,
    wraw,
    wwide,
    wflat,
    xn,
    acc,
    squares,
    text,
    scales,
    part,
    ybuf,
    zbuf,
    isums,
    tsums,
    xsend,
    xsums,
    table,
    kinv,
    starts,
    *rest,
):
    replicas, owners, tensors, positions = sizes
    group_tiles = 2 * owners
    proj, tiles, slots, inc, vit = (rest[i * CHUNKS : (i + 1) * CHUNKS] for i in range(5))
    zs, zr, xs, xr, ys, yr, zss, zsr, xss, xsr, tss, tsr, tsem, vsem, wsem, psem, osem = rest[5 * CHUNKS :]
    width, block = vit_hbm.shape[2], gain.shape[1]
    steps = width // DEPTH
    me_dp, me_s, me_t = lax.axis_index("dp"), lax.axis_index("seq"), lax.axis_index("tensor")

    def peer(me, k, n):
        return lax.rem(me + k, n)

    small = []
    for i, (source, target) in enumerate(
        (
            (ln_gain_hbm, ln_gain),
            (ln_bias_hbm, ln_bias),
            (bias_hbm, bias),
            (gain_hbm, gain),
            (dest_hbm, dest),
            (place_hbm, place),
        )
    ):
        small.append(pltpu.make_async_copy(source, target, psem.at[i]))
        small[-1].start()
    base = [sum(SPANS[:h]) for h in range(CHUNKS)]
    load_vit = []
    for h in range(CHUNKS):
        here = pl.ds(base[h], SPANS[h])
        load_vit.append(
            pltpu.make_async_copy(vit_hbm.at[:, here, :], vit[h], vsem.at[h])
        )
    load_vit[0].start()
    load_weight = []
    for i in range(steps):
        here = pl.ds(i * DEPTH * owners, DEPTH * owners)
        load_weight.append(
            pltpu.make_async_copy(weight_hbm.at[here], wraw.at[here], wsem.at[i])
        )
        load_weight[-1].start()
    for h in range(1, CHUNKS):
        load_vit[h].start()
    load_text = pltpu.make_async_copy(text_hbm, text, tsem)
    load_text.start()
    barrier = pltpu.get_barrier_semaphore()
    axes = (("dp", me_dp, replicas), ("seq", me_s, owners), ("tensor", me_t, tensors))
    for name, me, n in axes:
        for k in spiral(n):
            pl.semaphore_signal(
                barrier, inc=1, device_id={name: peer(me, k, n)}, device_id_type=MESH
            )

    def norm_chunk(h, side, first):
        load_vit[h].wait()

        def norm(g, carry):
            for i in range(2):
                rows = pl.ds(pl.multiple_of(16 * g, 16), 16)
                values = vit[h][i, rows, :].astype(jnp.float32)
                center = values - jnp.mean(values, axis=-1, keepdims=True)
                spread = jnp.mean(center * center, axis=-1, keepdims=True)
                normed = center * lax.rsqrt(spread + 1e-06) * lgain[...] + lbias[...]
                to = pl.ds(pl.multiple_of(first + i * SPANS[h] + 16 * g, 16), 16)
                xn[side, to, :] = normed.astype(jnp.bfloat16)
            return carry

        lax.fori_loop(0, SPANS[h] // 16, norm, 0)

    def keep(h, s, hidden):
        rounded = (hidden + bias[s : s + 1, :]).astype(jnp.bfloat16)
        proj[h][s] = rounded.reshape(2, SPANS[h], block)
        values = rounded.astype(jnp.float32)
        return (values * values).reshape(2, SPANS[h], block)


    def send_owners(h):
        for k in spiral(owners):
            to = peer(me_s, k, owners)
            pltpu.make_async_remote_copy(
                src_ref=proj[h].at[to],
                dst_ref=tiles[h].at[pl.ds(2 * me_s, 2)],
                send_sem=zs,
                recv_sem=zr.at[h, k],
                device_id={"seq": to},
                device_id_type=MESH,
            ).start()
        tiles[h][pl.ds(2 * me_s, 2)] = proj[h][me_s]

    small[0].wait()
    small[1].wait()
    for i in range(width // block):
        here = slice(i * block, (i + 1) * block)
        lgain[:, here] = ln_gain[i : i + 1, :]
        lbias[:, here] = ln_bias[i : i + 1, :]

    norm_chunk(0, 0, 0)
    first_rows = 2 * SPANS[0]

    def widen(i):
        load_weight[i].wait()
        here = pl.ds(i * DEPTH * owners, DEPTH * owners)
        wwide[i % 2] = wraw[here, :].astype(jnp.float32)

    widen(0)
    for i in range(steps):
        if i + 1 < steps:
            widen(i + 1)
        parts = [
            wwide[i % 2, pl.ds(s, DEPTH, stride=owners), :].astype(jnp.bfloat16)
            for s in range(owners)
        ]
        flat = jnp.concatenate(parts, axis=1)
        wflat[i * DEPTH : (i + 1) * DEPTH, :] = flat
        step = jnp.dot(
            xn[0, :first_rows, i * DEPTH : (i + 1) * DEPTH],
            flat,
            preferred_element_type=jnp.float32,
        )
        if i == 0:
            acc[...] = step
        else:
            acc[...] += step
    small[2].wait()
    total = jnp.zeros((2, SPANS[0], block), jnp.float32)
    for s in range(owners):
        total = total + keep(0, s, acc[:, s * block : (s + 1) * block])
    squares[:, 0 : SPANS[0], :] = total
    pl.semaphore_wait(barrier, replicas + owners + tensors - 3)
    send_owners(0)

    half = owners // 2

    def project(n_pass):
        rows = 0
        for h in PASSES[n_pass]:
            norm_chunk(h, n_pass % 2, rows)
            rows += 2 * SPANS[h]
        totals = [jnp.zeros((2, SPANS[h], block), jnp.float32) for h in PASSES[n_pass]]
        for n in range(2):
            hidden = jnp.dot(
                xn[n_pass % 2, :rows, :],
                wflat[:, n * half * block : (n + 1) * half * block],
                preferred_element_type=jnp.float32,
            )
            first = 0
            for i, h in enumerate(PASSES[n_pass]):
                mine = hidden[first : first + 2 * SPANS[h]]
                first += 2 * SPANS[h]
                for s in range(half):
                    columns = mine[:, s * block : (s + 1) * block]
                    totals[i] = totals[i] + keep(h, n * half + s, columns)
        for i, h in enumerate(PASSES[n_pass]):
            squares[:, base[h] : base[h] + SPANS[h], :] = totals[i]
            send_owners(h)

    for copy in small[3:]:
        copy.wait()
    for r in range(replicas):
        first = jnp.int32(group_tiles - 1)
        last = jnp.int32(0)
        for j in range(group_tiles):
            hit = dest[me_dp * group_tiles + j] == r
            last = jnp.where(hit, j, last)
            hit_back = dest[me_dp * group_tiles + group_tiles - 1 - j] == r
            first = jnp.where(hit_back, group_tiles - 1 - j, first)
        table[2 * r] = first
        table[2 * r + 1] = last

    for n_pass in range(1, EARLY):
        project(n_pass)


    def send_chunk(h):
        for k in range(1, owners):
            wait_for(tiles[h].at[pl.ds(2 * peer(me_s, owners - k, owners), 2)], zr.at[h, k])
        for k in spiral(replicas) + [0]:
            r = peer(me_dp, k, replicas)
            for c in range(CAP):
                slots[h][2 * r + c] = tiles[h][table[2 * r + c]]
        for k in spiral(replicas):
            to = peer(me_dp, k, replicas)
            pltpu.make_async_remote_copy(
                src_ref=slots[h].at[pl.ds(2 * to, 2)],
                dst_ref=inc[h].at[pl.ds(2 * me_dp, 2)],
                send_sem=xs,
                recv_sem=xr.at[h, k],
                device_id={"dp": to},
                device_id_type=MESH,
            ).start()
        inc[h][pl.ds(2 * me_dp, 2)] = slots[h][pl.ds(2 * me_dp, 2)]

    load_text.wait()
    sub = lax.broadcasted_iota(jnp.int32, (8, TILE), 0)
    share = positions // tensors

    def sum_text(t, carry):
        values = text[pl.ds(share * t, share)].astype(jnp.float32).reshape(share * TILE, TILE)
        sums = lane_sums(values * values)
        total = jnp.zeros((8, TILE), jnp.float32)
        for i in range(share):
            total = jnp.where(sub == i, sums[:, i * TILE : (i + 1) * TILE], total)
        part[t] = total
        return carry

    lax.fori_loop(0, tensors, sum_text, 0)
    send_chunk(0)
    for n_pass in range(EARLY, len(PASSES)):
        project(n_pass)
    sums = lane_sums(squares[...].reshape(2 * TILE, TILE))
    for t in range(tensors):
        for i in range(2):
            part[t, share + i : share + i + 1, :] = sums[:1, i * TILE : (i + 1) * TILE]
    for k in spiral(tensors):
        to = peer(me_t, k, tensors)
        pltpu.make_async_remote_copy(
            src_ref=part.at[to],
            dst_ref=ybuf.at[me_t],
            send_sem=ys,
            recv_sem=yr.at[k],
            device_id={"tensor": to},
            device_id_type=MESH,
        ).start()

    send_chunk(1)

    def count(g, total):
        starts[g] = total
        for j in range(group_tiles):
            total = total + jnp.where(dest[g * group_tiles + j] == me_dp, 1, 0)
        return total

    starts[replicas] = lax.fori_loop(0, replicas, count, jnp.int32(0))

    def invert(p, carry):
        order = jnp.int32(0)
        for k in range(positions):
            order = jnp.where(place[me_dp, k] == p, k, order)
        slot = jnp.int32(-1)
        for g in range(replicas):
            here = (order >= starts[g]) & (order < starts[g + 1])
            slot = jnp.where(here, 2 * g + order - starts[g], slot)
        kinv[p] = slot
        return carry

    lax.fori_loop(0, positions, invert, 0)

    for k in range(1, tensors):
        wait_for(ybuf.at[peer(me_t, tensors - k, tensors)], yr.at[k])
    ybuf[me_t] = part[me_t]
    total = ybuf[0]
    for t in range(1, tensors):
        total = total + ybuf[t]
    zbuf[me_s] = total
    for k in spiral(owners):
        to = peer(me_s, k, owners)
        pltpu.make_async_remote_copy(
            src_ref=zbuf.at[me_s],
            dst_ref=zbuf.at[me_s],
            send_sem=zss,
            recv_sem=zsr.at[k],
            device_id={"seq": to},
            device_id_type=MESH,
        ).start()

    send_chunk(2)

    for k in range(1, owners):
        wait_for(zbuf.at[peer(me_s, owners - k, owners)], zsr.at[k])
    for s in range(owners):
        isums[2 * s : 2 * s + 2, :] = zbuf[s, share : share + 2]
    for r in range(replicas):
        for c in range(CAP):
            xsend[r, c : c + 1, :] = isums[pl.ds(table[2 * r + c], 1), :]
    for k in spiral(replicas):
        to = peer(me_dp, k, replicas)
        pltpu.make_async_remote_copy(
            src_ref=xsend.at[to],
            dst_ref=xsums.at[me_dp],
            send_sem=xss,
            recv_sem=xsr.at[k],
            device_id={"dp": to},
            device_id_type=MESH,
        ).start()
    text_total = zbuf[0]
    for s in range(1, owners):
        text_total = text_total + zbuf[s]
    tsums[me_t] = text_total
    for k in spiral(tensors):
        to = peer(me_t, k, tensors)
        pltpu.make_async_remote_copy(
            src_ref=tsums.at[me_t],
            dst_ref=tsums.at[me_t],
            send_sem=tss,
            recv_sem=tsr.at[k],
            device_id={"tensor": to},
            device_id_type=MESH,
        ).start()
    for h in range(3, CHUNKS):
        send_chunk(h)
    xsums[me_dp] = xsend[me_dp]
    for k in range(1, tensors):
        wait_for(tsums.at[peer(me_t, tensors - k, tensors)], tsr.at[k])
    for k in range(1, replicas):
        wait_for(xsums.at[peer(me_dp, replicas - k, replicas)], xsr.at[k])

    def scale_rows(q, carry):
        for i in range(UNROLL):
            p = q * UNROLL + i
            slot = kinv[p]
            safe = jnp.maximum(slot, 0)
            image = xsums[safe // 2, pl.ds(lax.rem(safe, 2), 1), :]
            total = jnp.where(slot >= 0, image, tsums[p // share, pl.ds(lax.rem(p, share), 1), :])
            scale = lax.rsqrt(total / D + 1e-05)
            scales[p] = jnp.transpose(jnp.broadcast_to(scale, (TILE, TILE)))
        return carry

    lax.fori_loop(0, positions // UNROLL, scale_rows, 0)

    stores = []
    for h in range(CHUNKS):
        for k in range(1, replicas):
            slot = CAP * peer(me_dp, replicas - k, replicas)
            wait_for(inc[h].at[pl.ds(slot, CAP)], xr.at[h, k])

        here = pl.ds(base[h], SPANS[h])

        def finish(q, carry, h=h, here=here):
            for i in range(UNROLL):
                p = q * UNROLL + i
                slot = kinv[p]
                picked = inc[h][jnp.maximum(slot, 0)]
                chosen = jnp.where(slot >= 0, picked, text[p, here, :]).astype(jnp.float32)
                out[p, here, :] = (chosen * scales[p, here, :] * gain[...]).astype(jnp.bfloat16)
            return carry

        lax.fori_loop(0, positions // UNROLL, finish, 0)
        stores.append(
            pltpu.make_async_copy(out.at[:, here, :], out_hbm.at[:, here, :], osem.at[h])
        )
        stores[-1].start()

    wait_for(text.at[pl.ds(0, 2 * (owners - 1))], zs)
    wait_for(text.at[pl.ds(0, CAP * (replicas - 1))], xs)
    wait_for(ybuf.at[pl.ds(0, tensors - 1)], ys)
    wait_for(zbuf.at[pl.ds(0, owners - 1)], zss)
    wait_for(xsums.at[pl.ds(0, replicas - 1)], xss)
    wait_for(tsums.at[pl.ds(0, tensors - 1)], tss)
    for copy in stores:
        copy.wait()


def local(
    vit_out, ln_gain, ln_bias, proj_weight, proj_bias, text_embed, norm_gain, tile_dest, tile_place
):
    replicas, owners, tensors = (lax.axis_size(a) for a in ("dp", "seq", "tensor"))
    width = vit_out.shape[1]
    block = proj_weight.shape[2]
    positions = tile_place.shape[1]
    text = text_embed.reshape(positions, TILE, block)

    hbm = pl.BlockSpec(memory_space=pltpu.HBM)
    bf16, f32, i32 = jnp.bfloat16, jnp.float32, jnp.int32
    dma = pltpu.SemaphoreType.DMA

    def chunked(shape):
        return [pltpu.VMEM((*shape, span, block), bf16) for span in SPANS]

    out = pl.pallas_call(
        functools.partial(exchange_kernel, (replicas, owners, tensors, positions)),
        out_shape=jax.ShapeDtypeStruct(text.shape, bf16),
        in_specs=[hbm] * 9,
        out_specs=hbm,
        scratch_shapes=[
            pltpu.VMEM(text.shape, bf16),
            pltpu.VMEM((width // block, block), f32),
            pltpu.VMEM((width // block, block), f32),
            pltpu.VMEM(proj_bias.shape, f32),
            pltpu.VMEM((1, block), f32),
            pltpu.SMEM((tile_dest.shape[0],), i32),
            pltpu.SMEM(tile_place.shape, i32),
            pltpu.VMEM((1, width), f32),
            pltpu.VMEM((1, width), f32),
            pltpu.VMEM((width * owners, block), bf16),
            pltpu.VMEM((2, DEPTH * owners, block), f32),
            pltpu.VMEM((width, owners * block), bf16),
            pltpu.VMEM((2, 2 * max(sum(SPANS[h] for h in p) for p in PASSES), width), bf16),
            pltpu.VMEM((2 * SPANS[0], owners * block), f32),
            pltpu.VMEM((2, TILE, block), f32),
            pltpu.VMEM(text.shape, bf16),
            pltpu.VMEM(text.shape, f32),
            pltpu.VMEM((tensors, 8, TILE), f32),
            pltpu.VMEM((tensors, 8, TILE), f32),
            pltpu.VMEM((owners, 8, TILE), f32),
            pltpu.VMEM((2 * owners, TILE), f32),
            pltpu.VMEM((tensors, 8, TILE), f32),
            pltpu.VMEM((replicas, 8, TILE), f32),
            pltpu.VMEM((replicas, 8, TILE), f32),
            pltpu.SMEM((CAP * replicas,), i32),
            pltpu.SMEM((positions,), i32),
            pltpu.SMEM((replicas + 1,), i32),
        ]
        + chunked((owners, 2))
        + chunked((2 * owners,))
        + chunked((CAP * replicas,))
        + chunked((CAP * replicas,))
        + [pltpu.VMEM((2, span, width), bf16) for span in SPANS]
        + [dma, dma((CHUNKS, owners)), dma, dma((CHUNKS, replicas))]
        + [dma, dma((tensors,)), dma, dma((owners,))]
        + [dma, dma((replicas,)), dma, dma((tensors,))]
        + [dma, dma((CHUNKS,)), dma((width // DEPTH,)), dma((6,)), dma((CHUNKS,))],
        compiler_params=pltpu.CompilerParams(
            collective_id=0, has_side_effects=True, vmem_limit_bytes=LIMIT * 1024 * 1024
        ),
    )(
        vit_out.reshape(2, TILE, width),
        proj_weight.reshape(width * owners, block),
        ln_gain.reshape(-1, block),
        ln_bias.reshape(-1, block),
        proj_bias,
        text,
        norm_gain.reshape(1, block),
        tile_dest.reshape(-1),
        tile_place,
    )
    return out.reshape(text_embed.shape)


def solution(mesh):
    placed = (
        P(("dp", "seq"), None),
        P(),
        P(),
        P(None, None, "tensor"),
        P(None, "tensor"),
        P("dp", ("seq", "tensor")),
        P(("seq", "tensor")),
        P(),
        P(),
    )
    return jax.shard_map(
        local, mesh=mesh, in_specs=placed, out_specs=P("dp", ("seq", "tensor")), check_vma=False
    )
```

```python
import functools

import jax
import jax.numpy as jnp
from jax import lax
from jax.experimental import pallas as pl
from jax.experimental.pallas import tpu as pltpu
from jax.sharding import PartitionSpec as P

D = 8192
TILE = 128
CAP = 2
SPANS = (16, 16, 32, 32, 32)
CHUNKS = len(SPANS)
DEPTH = 640
LIMIT = 56
PASSES = ((0,), (1,), (2,), (3, 4))
EARLY = 3
UNROLL = 4
MESH = pl.DeviceIdType.MESH


def spiral(n):
    order = [n // 2]
    for d in range(n // 2 - 1, 0, -1):
        order += [d, n - d]
    return order


def wait_for(ref, sem):
    pltpu.make_async_copy(ref, ref, sem).wait()


def lane_sums(squares):
    ones = jnp.ones((8, squares.shape[1]), jnp.bfloat16)
    dims = (((1,), (1,)), ((), ()))
    high = squares.astype(jnp.bfloat16)
    low = (squares - high.astype(jnp.float32)).astype(jnp.bfloat16)
    return lax.dot_general(
        ones, high, dims, preferred_element_type=jnp.float32
    ) + lax.dot_general(ones, low, dims, preferred_element_type=jnp.float32)


def exchange_kernel(
    sizes,
    vit_hbm,
    weight_hbm,
    ln_gain_hbm,
    ln_bias_hbm,
    bias_hbm,
    text_hbm,
    gain_hbm,
    dest_hbm,
    place_hbm,
    out_hbm,
    out,
    ln_gain,
    ln_bias,
    bias,
    gain,
    dest,
    place,
    lgain,
    lbias,
    wraw,
    wwide,
    wflat,
    xn,
    acc,
    squares,
    text,
    scales,
    part,
    ybuf,
    zbuf,
    isums,
    tsums,
    xsend,
    xsums,
    table,
    kinv,
    starts,
    *rest,
):
    replicas, owners, tensors, positions = sizes
    group_tiles = 2 * owners
    proj, tiles, slots, inc, vit = (rest[i * CHUNKS : (i + 1) * CHUNKS] for i in range(5))
    zs, zr, xs, xr, ys, yr, zss, zsr, xss, xsr, tss, tsr, tsem, vsem, wsem, psem, osem = rest[5 * CHUNKS :]
    width, block = vit_hbm.shape[2], gain.shape[1]
    steps = width // DEPTH
    me_dp, me_s, me_t = lax.axis_index("dp"), lax.axis_index("seq"), lax.axis_index("tensor")

    def peer(me, k, n):
        return lax.rem(me + k, n)

    small = []
    for i, (source, target) in enumerate(
        (
            (ln_gain_hbm, ln_gain),
            (ln_bias_hbm, ln_bias),
            (bias_hbm, bias),
            (gain_hbm, gain),
            (dest_hbm, dest),
            (place_hbm, place),
        )
    ):
        small.append(pltpu.make_async_copy(source, target, psem.at[i]))
    base = [sum(SPANS[:h]) for h in range(CHUNKS)]
    load_vit = []
    for h in range(CHUNKS):
        here = pl.ds(base[h], SPANS[h])
        load_vit.append(
            pltpu.make_async_copy(vit_hbm.at[:, here, :], vit[h], vsem.at[h])
        )
    load_vit[0].start()
    for copy in small[:3]:
        copy.start()
    load_weight = []
    for i in range(steps):
        here = pl.ds(i * DEPTH * owners, DEPTH * owners)
        load_weight.append(
            pltpu.make_async_copy(weight_hbm.at[here], wraw.at[here], wsem.at[i])
        )
    for copy in load_weight:
        copy.start()
    for copy in small[3:]:
        copy.start()
    load_text = pltpu.make_async_copy(text_hbm, text, tsem)
    barrier = pltpu.get_barrier_semaphore()
    axes = (("dp", me_dp, replicas), ("seq", me_s, owners), ("tensor", me_t, tensors))
    for name, me, n in axes:
        for k in spiral(n):
            pl.semaphore_signal(
                barrier, inc=1, device_id={name: peer(me, k, n)}, device_id_type=MESH
            )

    def norm_chunk(h, side, first):
        load_vit[h].wait()

        def norm(g, carry):
            for i in range(2):
                rows = pl.ds(pl.multiple_of(16 * g, 16), 16)
                values = vit[h][i, rows, :].astype(jnp.float32)
                center = values - jnp.mean(values, axis=-1, keepdims=True)
                spread = jnp.mean(center * center, axis=-1, keepdims=True)
                normed = center * lax.rsqrt(spread + 1e-06) * lgain[...] + lbias[...]
                to = pl.ds(pl.multiple_of(first + i * SPANS[h] + 16 * g, 16), 16)
                xn[side, to, :] = normed.astype(jnp.bfloat16)
            return carry

        lax.fori_loop(0, SPANS[h] // 16, norm, 0)

    def keep(h, s, hidden):
        rounded = (hidden + bias[s : s + 1, :]).astype(jnp.bfloat16)
        proj[h][s] = rounded.reshape(2, SPANS[h], block)
        values = rounded.astype(jnp.float32)
        return (values * values).reshape(2, SPANS[h], block)


    def send_owners(h):
        for k in spiral(owners):
            to = peer(me_s, k, owners)
            pltpu.make_async_remote_copy(
                src_ref=proj[h].at[to],
                dst_ref=tiles[h].at[pl.ds(2 * me_s, 2)],
                send_sem=zs,
                recv_sem=zr.at[h],
                device_id={"seq": to},
                device_id_type=MESH,
            ).start()
        tiles[h][pl.ds(2 * me_s, 2)] = proj[h][me_s]

    small[0].wait()
    small[1].wait()
    for i in range(width // block):
        here = slice(i * block, (i + 1) * block)
        lgain[:, here] = ln_gain[i : i + 1, :]
        lbias[:, here] = ln_bias[i : i + 1, :]

    norm_chunk(0, 0, 0)
    first_rows = 2 * SPANS[0]

    def widen(i):
        load_weight[i].wait()
        if i == max(0, steps - 2):
            for copy in load_vit[1:]:
                copy.start()
            load_text.start()
        here = pl.ds(i * DEPTH * owners, DEPTH * owners)
        wwide[i % 2] = wraw[here, :].astype(jnp.float32)

    widen(0)
    for i in range(steps):
        if i + 1 < steps:
            widen(i + 1)
        parts = [
            wwide[i % 2, pl.ds(s, DEPTH, stride=owners), :].astype(jnp.bfloat16)
            for s in range(owners)
        ]
        flat = jnp.concatenate(parts, axis=1)
        wflat[i * DEPTH : (i + 1) * DEPTH, :] = flat
        step = jnp.dot(
            xn[0, :first_rows, i * DEPTH : (i + 1) * DEPTH],
            flat,
            preferred_element_type=jnp.float32,
        )
        if i == 0:
            acc[...] = step
        else:
            acc[...] += step
    small[2].wait()
    total = jnp.zeros((2, SPANS[0], block), jnp.float32)
    for s in range(owners):
        total = total + keep(0, s, acc[:, s * block : (s + 1) * block])
    squares[:, 0 : SPANS[0], :] = total
    pl.semaphore_wait(barrier, replicas + owners + tensors - 3)
    send_owners(0)

    half = owners // 2

    def project(n_pass):
        rows = 0
        for h in PASSES[n_pass]:
            norm_chunk(h, n_pass % 2, rows)
            rows += 2 * SPANS[h]
        totals = [jnp.zeros((2, SPANS[h], block), jnp.float32) for h in PASSES[n_pass]]
        for n in range(2):
            hidden = jnp.dot(
                xn[n_pass % 2, :rows, :],
                wflat[:, n * half * block : (n + 1) * half * block],
                preferred_element_type=jnp.float32,
            )
            first = 0
            for i, h in enumerate(PASSES[n_pass]):
                mine = hidden[first : first + 2 * SPANS[h]]
                first += 2 * SPANS[h]
                for s in range(half):
                    columns = mine[:, s * block : (s + 1) * block]
                    totals[i] = totals[i] + keep(h, n * half + s, columns)
        for i, h in enumerate(PASSES[n_pass]):
            squares[:, base[h] : base[h] + SPANS[h], :] = totals[i]
            send_owners(h)

    for copy in small[3:]:
        copy.wait()
    for r in range(replicas):
        first = jnp.int32(group_tiles - 1)
        last = jnp.int32(0)
        for j in range(group_tiles):
            hit = dest[me_dp * group_tiles + j] == r
            last = jnp.where(hit, j, last)
            hit_back = dest[me_dp * group_tiles + group_tiles - 1 - j] == r
            first = jnp.where(hit_back, group_tiles - 1 - j, first)
        table[2 * r] = first
        table[2 * r + 1] = last

    for n_pass in range(1, EARLY):
        project(n_pass)


    def send_chunk(h):
        wait_for(tiles[h].at[pl.ds(0, 2 * (owners - 1))], zr.at[h])
        for k in spiral(replicas) + [0]:
            r = peer(me_dp, k, replicas)
            for c in range(CAP):
                slots[h][2 * r + c] = tiles[h][table[2 * r + c]]
        for k in spiral(replicas):
            to = peer(me_dp, k, replicas)
            pltpu.make_async_remote_copy(
                src_ref=slots[h].at[pl.ds(2 * to, 2)],
                dst_ref=inc[h].at[pl.ds(2 * me_dp, 2)],
                send_sem=xs,
                recv_sem=xr.at[h],
                device_id={"dp": to},
                device_id_type=MESH,
            ).start()
        inc[h][pl.ds(2 * me_dp, 2)] = slots[h][pl.ds(2 * me_dp, 2)]

    load_text.wait()
    sub = lax.broadcasted_iota(jnp.int32, (8, TILE), 0)
    share = positions // tensors

    def sum_text(t, carry):
        values = text[pl.ds(share * t, share)].astype(jnp.float32).reshape(share * TILE, TILE)
        sums = lane_sums(values * values)
        total = jnp.zeros((8, TILE), jnp.float32)
        for i in range(share):
            total = jnp.where(sub == i, sums[:, i * TILE : (i + 1) * TILE], total)
        part[t] = total
        return carry

    lax.fori_loop(0, tensors, sum_text, 0)
    send_chunk(0)
    for n_pass in range(EARLY, len(PASSES)):
        project(n_pass)
    sums = lane_sums(squares[...].reshape(2 * TILE, TILE))
    for t in range(tensors):
        for i in range(2):
            part[t, share + i : share + i + 1, :] = sums[:1, i * TILE : (i + 1) * TILE]
    for k in spiral(tensors):
        to = peer(me_t, k, tensors)
        pltpu.make_async_remote_copy(
            src_ref=part.at[to],
            dst_ref=ybuf.at[me_t],
            send_sem=ys,
            recv_sem=yr,
            device_id={"tensor": to},
            device_id_type=MESH,
        ).start()

    send_chunk(1)

    def count(g, total):
        starts[g] = total
        for j in range(group_tiles):
            total = total + jnp.where(dest[g * group_tiles + j] == me_dp, 1, 0)
        return total

    starts[replicas] = lax.fori_loop(0, replicas, count, jnp.int32(0))

    def invert(p, carry):
        order = jnp.int32(0)
        for k in range(positions):
            order = jnp.where(place[me_dp, k] == p, k, order)
        slot = jnp.int32(-1)
        for g in range(replicas):
            here = (order >= starts[g]) & (order < starts[g + 1])
            slot = jnp.where(here, 2 * g + order - starts[g], slot)
        kinv[p] = slot
        return carry

    lax.fori_loop(0, positions, invert, 0)

    wait_for(ybuf.at[pl.ds(0, tensors - 1)], yr)
    ybuf[me_t] = part[me_t]
    total = ybuf[0]
    for t in range(1, tensors):
        total = total + ybuf[t]
    zbuf[me_s] = total
    for k in spiral(owners):
        to = peer(me_s, k, owners)
        pltpu.make_async_remote_copy(
            src_ref=zbuf.at[me_s],
            dst_ref=zbuf.at[me_s],
            send_sem=zss,
            recv_sem=zsr,
            device_id={"seq": to},
            device_id_type=MESH,
        ).start()

    send_chunk(2)

    wait_for(zbuf.at[pl.ds(0, owners - 1)], zsr)
    for s in range(owners):
        isums[2 * s : 2 * s + 2, :] = zbuf[s, share : share + 2]
    for r in range(replicas):
        for c in range(CAP):
            xsend[r, c : c + 1, :] = isums[pl.ds(table[2 * r + c], 1), :]
    for k in spiral(replicas):
        to = peer(me_dp, k, replicas)
        pltpu.make_async_remote_copy(
            src_ref=xsend.at[to],
            dst_ref=xsums.at[me_dp],
            send_sem=xss,
            recv_sem=xsr,
            device_id={"dp": to},
            device_id_type=MESH,
        ).start()
    text_total = zbuf[0]
    for s in range(1, owners):
        text_total = text_total + zbuf[s]
    tsums[me_t] = text_total
    for k in spiral(tensors):
        to = peer(me_t, k, tensors)
        pltpu.make_async_remote_copy(
            src_ref=tsums.at[me_t],
            dst_ref=tsums.at[me_t],
            send_sem=tss,
            recv_sem=tsr,
            device_id={"tensor": to},
            device_id_type=MESH,
        ).start()
    for h in range(3, CHUNKS):
        send_chunk(h)
    xsums[me_dp] = xsend[me_dp]
    wait_for(tsums.at[pl.ds(0, tensors - 1)], tsr)
    wait_for(xsums.at[pl.ds(0, replicas - 1)], xsr)

    def scale_rows(q, carry):
        for i in range(UNROLL):
            p = q * UNROLL + i
            slot = kinv[p]
            safe = jnp.maximum(slot, 0)
            image = xsums[safe // 2, pl.ds(lax.rem(safe, 2), 1), :]
            total = jnp.where(slot >= 0, image, tsums[p // share, pl.ds(lax.rem(p, share), 1), :])
            scale = lax.rsqrt(total / D + 1e-05)
            scales[p] = jnp.transpose(jnp.broadcast_to(scale, (TILE, TILE)))
        return carry

    lax.fori_loop(0, positions // UNROLL, scale_rows, 0)

    stores = []
    for h in range(CHUNKS):
        wait_for(inc[h].at[pl.ds(0, CAP * (replicas - 1))], xr.at[h])

        here = pl.ds(base[h], SPANS[h])

        def finish(q, carry, h=h, here=here):
            for i in range(UNROLL):
                p = q * UNROLL + i
                slot = kinv[p]
                picked = inc[h][jnp.maximum(slot, 0)]
                chosen = jnp.where(slot >= 0, picked, text[p, here, :]).astype(jnp.float32)
                out[p, here, :] = (chosen * scales[p, here, :] * gain[...]).astype(jnp.bfloat16)
            return carry

        lax.fori_loop(0, positions // UNROLL, finish, 0)
        stores.append(
            pltpu.make_async_copy(out.at[:, here, :], out_hbm.at[:, here, :], osem.at[h])
        )
        stores[-1].start()

    wait_for(text.at[pl.ds(0, 2 * (owners - 1))], zs)
    wait_for(text.at[pl.ds(0, CAP * (replicas - 1))], xs)
    wait_for(ybuf.at[pl.ds(0, tensors - 1)], ys)
    wait_for(zbuf.at[pl.ds(0, owners - 1)], zss)
    wait_for(xsums.at[pl.ds(0, replicas - 1)], xss)
    wait_for(tsums.at[pl.ds(0, tensors - 1)], tss)
    for copy in stores:
        copy.wait()


def copy_kernel(source, target, held, in_sem, out_sem):
    parts = in_sem.shape[0]
    rows = held.shape[0] // parts
    loads, stores = [], []
    for i in range(parts):
        here = pl.ds(i * rows, rows)
        loads.append(pltpu.make_async_copy(source.at[here], held.at[here], in_sem.at[i]))
        stores.append(pltpu.make_async_copy(held.at[here], target.at[here], out_sem.at[i]))
        loads[-1].start()
    for load, store in zip(loads, stores):
        load.wait()
        store.start()
    for store in stores:
        store.wait()


def local(
    vit_out, ln_gain, ln_bias, proj_weight, proj_bias, text_embed, norm_gain, tile_dest, tile_place
):
    replicas, owners, tensors = (lax.axis_size(a) for a in ("dp", "seq", "tensor"))
    width = vit_out.shape[1]
    block = proj_weight.shape[2]
    positions = tile_place.shape[1]
    text = text_embed.reshape(positions, TILE, block)

    hbm = pl.BlockSpec(memory_space=pltpu.HBM)
    bf16, f32, i32 = jnp.bfloat16, jnp.float32, jnp.int32
    dma = pltpu.SemaphoreType.DMA

    def chunked(shape):
        return [pltpu.VMEM((*shape, span, block), bf16) for span in SPANS]

    out = pl.pallas_call(
        functools.partial(exchange_kernel, (replicas, owners, tensors, positions)),
        out_shape=jax.ShapeDtypeStruct(text.shape, bf16),
        in_specs=[hbm] * 9,
        out_specs=hbm,
        scratch_shapes=[
            pltpu.VMEM(text.shape, bf16),
            pltpu.VMEM((width // block, block), f32),
            pltpu.VMEM((width // block, block), f32),
            pltpu.VMEM(proj_bias.shape, f32),
            pltpu.VMEM((1, block), f32),
            pltpu.SMEM((tile_dest.shape[0],), i32),
            pltpu.SMEM(tile_place.shape, i32),
            pltpu.VMEM((1, width), f32),
            pltpu.VMEM((1, width), f32),
            pltpu.VMEM((width * owners, block), bf16),
            pltpu.VMEM((2, DEPTH * owners, block), f32),
            pltpu.VMEM((width, owners * block), bf16),
            pltpu.VMEM((2, 2 * max(sum(SPANS[h] for h in p) for p in PASSES), width), bf16),
            pltpu.VMEM((2 * SPANS[0], owners * block), f32),
            pltpu.VMEM((2, TILE, block), f32),
            pltpu.VMEM(text.shape, bf16),
            pltpu.VMEM(text.shape, f32),
            pltpu.VMEM((tensors, 8, TILE), f32),
            pltpu.VMEM((tensors, 8, TILE), f32),
            pltpu.VMEM((owners, 8, TILE), f32),
            pltpu.VMEM((2 * owners, TILE), f32),
            pltpu.VMEM((tensors, 8, TILE), f32),
            pltpu.VMEM((replicas, 8, TILE), f32),
            pltpu.VMEM((replicas, 8, TILE), f32),
            pltpu.SMEM((CAP * replicas,), i32),
            pltpu.SMEM((positions,), i32),
            pltpu.SMEM((replicas + 1,), i32),
        ]
        + chunked((owners, 2))
        + chunked((2 * owners,))
        + chunked((CAP * replicas,))
        + chunked((CAP * replicas,))
        + [pltpu.VMEM((2, span, width), bf16) for span in SPANS]
        + [dma, dma((CHUNKS,))] * 2
        + [dma] * 8
        + [dma, dma((CHUNKS,)), dma((width // DEPTH,)), dma((6,)), dma((CHUNKS,))],
        compiler_params=pltpu.CompilerParams(
            collective_id=0, has_side_effects=True, vmem_limit_bytes=LIMIT * 1024 * 1024
        ),
    )(
        vit_out.reshape(2, TILE, width),
        proj_weight.reshape(width * owners, block),
        ln_gain.reshape(-1, block),
        ln_bias.reshape(-1, block),
        proj_bias,
        text,
        norm_gain.reshape(1, block),
        tile_dest.reshape(-1),
        tile_place,
    )
    return pl.pallas_call(
        copy_kernel,
        out_shape=jax.ShapeDtypeStruct(text.shape, bf16),
        in_specs=[hbm],
        out_specs=hbm,
        scratch_shapes=[pltpu.VMEM(text.shape, bf16), dma((4,)), dma((4,))],
        compiler_params=pltpu.CompilerParams(vmem_limit_bytes=60 * 1024 * 1024),
    )(out).reshape(text_embed.shape)


def solution(mesh):
    placed = (
        P(("dp", "seq"), None),
        P(),
        P(),
        P(None, None, "tensor"),
        P(None, "tensor"),
        P("dp", ("seq", "tensor")),
        P(("seq", "tensor")),
        P(),
        P(),
    )
    return jax.shard_map(
        local, mesh=mesh, in_specs=placed, out_specs=P("dp", ("seq", "tensor")), check_vma=False
    )
```

```python
import functools

import jax
import jax.numpy as jnp
from jax import lax
from jax.experimental import pallas as pl
from jax.experimental.pallas import tpu as pltpu
from jax.sharding import PartitionSpec as P

D = 8192
TILE = 128
CAP = 2
SPANS = (16, 16, 32, 32, 32)
CHUNKS = len(SPANS)
DEPTH = 640
LIMIT = 56
PASSES = ((0,), (1,), (2,), (3, 4))
EARLY = 3
UNROLL = 4
MESH = pl.DeviceIdType.MESH


def spiral(n):
    order = [n // 2]
    for d in range(n // 2 - 1, 0, -1):
        order += [d, n - d]
    return order


def wait_for(ref, sem):
    pltpu.make_async_copy(ref, ref, sem).wait()


def lane_sums(squares):
    ones = jnp.ones((8, squares.shape[1]), jnp.bfloat16)
    dims = (((1,), (1,)), ((), ()))
    high = squares.astype(jnp.bfloat16)
    low = (squares - high.astype(jnp.float32)).astype(jnp.bfloat16)
    return lax.dot_general(
        ones, high, dims, preferred_element_type=jnp.float32
    ) + lax.dot_general(ones, low, dims, preferred_element_type=jnp.float32)


def exchange_kernel(
    sizes,
    vit_hbm,
    weight_hbm,
    ln_gain_hbm,
    ln_bias_hbm,
    bias_hbm,
    text_hbm,
    gain_hbm,
    dest_hbm,
    place_hbm,
    out_hbm,
    out,
    ln_gain,
    ln_bias,
    bias,
    gain,
    dest,
    place,
    lgain,
    lbias,
    wraw,
    wwide,
    wflat,
    xn,
    acc,
    squares,
    text,
    scales,
    part,
    ybuf,
    zbuf,
    isums,
    tsums,
    xsend,
    xsums,
    table,
    kinv,
    starts,
    *rest,
):
    replicas, owners, tensors, positions = sizes
    group_tiles = 2 * owners
    proj, tiles, slots, inc, vit = (rest[i * CHUNKS : (i + 1) * CHUNKS] for i in range(5))
    zs, zr, xs, xr, ys, yr, zss, zsr, xss, xsr, tss, tsr, tsem, vsem, wsem, psem, osem = rest[5 * CHUNKS :]
    width, block = vit_hbm.shape[2], gain.shape[1]
    steps = width // DEPTH
    me_dp, me_s, me_t = lax.axis_index("dp"), lax.axis_index("seq"), lax.axis_index("tensor")

    def peer(me, k, n):
        return lax.rem(me + k, n)

    small = []
    for i, (source, target) in enumerate(
        (
            (ln_gain_hbm, ln_gain),
            (ln_bias_hbm, ln_bias),
            (bias_hbm, bias),
            (gain_hbm, gain),
            (dest_hbm, dest),
            (place_hbm, place),
        )
    ):
        small.append(pltpu.make_async_copy(source, target, psem.at[i]))
        small[-1].start()
    base = [sum(SPANS[:h]) for h in range(CHUNKS)]
    load_vit = []
    for h in range(CHUNKS):
        here = pl.ds(base[h], SPANS[h])
        load_vit.append(
            pltpu.make_async_copy(vit_hbm.at[:, here, :], vit[h], vsem.at[h])
        )
    load_vit[0].start()
    load_weight = []
    for i in range(steps):
        here = pl.ds(i * DEPTH * owners, DEPTH * owners)
        load_weight.append(
            pltpu.make_async_copy(weight_hbm.at[here], wraw.at[here], wsem.at[i])
        )
    for copy in load_weight:
        copy.start()
    for copy in load_vit[1:]:
        copy.start()
    load_text = pltpu.make_async_copy(text_hbm, text, tsem)
    load_text.start()
    barrier = pltpu.get_barrier_semaphore()
    axes = (("dp", me_dp, replicas), ("seq", me_s, owners), ("tensor", me_t, tensors))
    for name, me, n in axes:
        for k in spiral(n):
            pl.semaphore_signal(
                barrier, inc=1, device_id={name: peer(me, k, n)}, device_id_type=MESH
            )

    def norm_chunk(h, side, first):
        load_vit[h].wait()

        def norm(g, carry):
            for i in range(2):
                rows = pl.ds(pl.multiple_of(16 * g, 16), 16)
                values = vit[h][i, rows, :].astype(jnp.float32)
                center = values - jnp.mean(values, axis=-1, keepdims=True)
                spread = jnp.mean(center * center, axis=-1, keepdims=True)
                normed = center * lax.rsqrt(spread + 1e-06) * lgain[...] + lbias[...]
                to = pl.ds(pl.multiple_of(first + i * SPANS[h] + 16 * g, 16), 16)
                xn[side, to, :] = normed.astype(jnp.bfloat16)
            return carry

        lax.fori_loop(0, SPANS[h] // 16, norm, 0)

    def keep(h, s, hidden):
        rounded = (hidden + bias[s : s + 1, :]).astype(jnp.bfloat16)
        proj[h][s] = rounded.reshape(2, SPANS[h], block)
        values = rounded.astype(jnp.float32)
        return (values * values).reshape(2, SPANS[h], block)


    def send_owners(h):
        for k in spiral(owners):
            to = peer(me_s, k, owners)
            pltpu.make_async_remote_copy(
                src_ref=proj[h].at[to],
                dst_ref=tiles[h].at[pl.ds(2 * me_s, 2)],
                send_sem=zs,
                recv_sem=zr.at[h],
                device_id={"seq": to},
                device_id_type=MESH,
            ).start()
        tiles[h][pl.ds(2 * me_s, 2)] = proj[h][me_s]

    small[0].wait()
    small[1].wait()
    for i in range(width // block):
        here = slice(i * block, (i + 1) * block)
        lgain[:, here] = ln_gain[i : i + 1, :]
        lbias[:, here] = ln_bias[i : i + 1, :]

    norm_chunk(0, 0, 0)
    first_rows = 2 * SPANS[0]

    def widen(i):
        load_weight[i].wait()
        here = pl.ds(i * DEPTH * owners, DEPTH * owners)
        wwide[i % 2] = wraw[here, :].astype(jnp.float32)

    widen(0)
    for i in range(steps):
        if i + 1 < steps:
            widen(i + 1)
        parts = [
            wwide[i % 2, pl.ds(s, DEPTH, stride=owners), :].astype(jnp.bfloat16)
            for s in range(owners)
        ]
        flat = jnp.concatenate(parts, axis=1)
        wflat[i * DEPTH : (i + 1) * DEPTH, :] = flat
        step = jnp.dot(
            xn[0, :first_rows, i * DEPTH : (i + 1) * DEPTH],
            flat,
            preferred_element_type=jnp.float32,
        )
        if i == 0:
            acc[...] = step
        else:
            acc[...] += step
    small[2].wait()
    total = jnp.zeros((2, SPANS[0], block), jnp.float32)
    for s in range(owners):
        total = total + keep(0, s, acc[:, s * block : (s + 1) * block])
    squares[:, 0 : SPANS[0], :] = total
    pl.semaphore_wait(barrier, replicas + owners + tensors - 3)
    send_owners(0)

    half = owners // 2

    def project(n_pass):
        rows = 0
        for h in PASSES[n_pass]:
            norm_chunk(h, n_pass % 2, rows)
            rows += 2 * SPANS[h]
        totals = [jnp.zeros((2, SPANS[h], block), jnp.float32) for h in PASSES[n_pass]]
        for n in range(2):
            hidden = jnp.dot(
                xn[n_pass % 2, :rows, :],
                wflat[:, n * half * block : (n + 1) * half * block],
                preferred_element_type=jnp.float32,
            )
            first = 0
            for i, h in enumerate(PASSES[n_pass]):
                mine = hidden[first : first + 2 * SPANS[h]]
                first += 2 * SPANS[h]
                for s in range(half):
                    columns = mine[:, s * block : (s + 1) * block]
                    totals[i] = totals[i] + keep(h, n * half + s, columns)
        for i, h in enumerate(PASSES[n_pass]):
            squares[:, base[h] : base[h] + SPANS[h], :] = totals[i]
            send_owners(h)

    for copy in small[3:]:
        copy.wait()
    for r in range(replicas):
        first = jnp.int32(group_tiles - 1)
        last = jnp.int32(0)
        for j in range(group_tiles):
            hit = dest[me_dp * group_tiles + j] == r
            last = jnp.where(hit, j, last)
            hit_back = dest[me_dp * group_tiles + group_tiles - 1 - j] == r
            first = jnp.where(hit_back, group_tiles - 1 - j, first)
        table[2 * r] = first
        table[2 * r + 1] = last

    for n_pass in range(1, EARLY):
        project(n_pass)


    def send_chunk(h):
        wait_for(tiles[h].at[pl.ds(0, 2 * (owners - 1))], zr.at[h])
        for k in spiral(replicas) + [0]:
            r = peer(me_dp, k, replicas)
            for c in range(CAP):
                slots[h][2 * r + c] = tiles[h][table[2 * r + c]]
        for k in spiral(replicas):
            to = peer(me_dp, k, replicas)
            pltpu.make_async_remote_copy(
                src_ref=slots[h].at[pl.ds(2 * to, 2)],
                dst_ref=inc[h].at[pl.ds(2 * me_dp, 2)],
                send_sem=xs,
                recv_sem=xr.at[h],
                device_id={"dp": to},
                device_id_type=MESH,
            ).start()
        inc[h][pl.ds(2 * me_dp, 2)] = slots[h][pl.ds(2 * me_dp, 2)]

    load_text.wait()
    sub = lax.broadcasted_iota(jnp.int32, (8, TILE), 0)
    share = positions // tensors

    def sum_text(t, carry):
        values = text[pl.ds(share * t, share)].astype(jnp.float32).reshape(share * TILE, TILE)
        sums = lane_sums(values * values)
        total = jnp.zeros((8, TILE), jnp.float32)
        for i in range(share):
            total = jnp.where(sub == i, sums[:, i * TILE : (i + 1) * TILE], total)
        part[t] = total
        return carry

    lax.fori_loop(0, tensors, sum_text, 0)
    send_chunk(0)
    for n_pass in range(EARLY, len(PASSES)):
        project(n_pass)
    sums = lane_sums(squares[...].reshape(2 * TILE, TILE))
    for t in range(tensors):
        for i in range(2):
            part[t, share + i : share + i + 1, :] = sums[:1, i * TILE : (i + 1) * TILE]
    for k in spiral(tensors):
        to = peer(me_t, k, tensors)
        pltpu.make_async_remote_copy(
            src_ref=part.at[to],
            dst_ref=ybuf.at[me_t],
            send_sem=ys,
            recv_sem=yr,
            device_id={"tensor": to},
            device_id_type=MESH,
        ).start()

    send_chunk(1)

    def count(g, total):
        starts[g] = total
        for j in range(group_tiles):
            total = total + jnp.where(dest[g * group_tiles + j] == me_dp, 1, 0)
        return total

    starts[replicas] = lax.fori_loop(0, replicas, count, jnp.int32(0))

    def invert(p, carry):
        order = jnp.int32(0)
        for k in range(positions):
            order = jnp.where(place[me_dp, k] == p, k, order)
        slot = jnp.int32(-1)
        for g in range(replicas):
            here = (order >= starts[g]) & (order < starts[g + 1])
            slot = jnp.where(here, 2 * g + order - starts[g], slot)
        kinv[p] = slot
        return carry

    lax.fori_loop(0, positions, invert, 0)

    wait_for(ybuf.at[pl.ds(0, tensors - 1)], yr)
    ybuf[me_t] = part[me_t]
    total = ybuf[0]
    for t in range(1, tensors):
        total = total + ybuf[t]
    zbuf[me_s] = total
    for k in spiral(owners):
        to = peer(me_s, k, owners)
        pltpu.make_async_remote_copy(
            src_ref=zbuf.at[me_s],
            dst_ref=zbuf.at[me_s],
            send_sem=zss,
            recv_sem=zsr,
            device_id={"seq": to},
            device_id_type=MESH,
        ).start()

    send_chunk(2)

    wait_for(zbuf.at[pl.ds(0, owners - 1)], zsr)
    for s in range(owners):
        isums[2 * s : 2 * s + 2, :] = zbuf[s, share : share + 2]
    for r in range(replicas):
        for c in range(CAP):
            xsend[r, c : c + 1, :] = isums[pl.ds(table[2 * r + c], 1), :]
    for k in spiral(replicas):
        to = peer(me_dp, k, replicas)
        pltpu.make_async_remote_copy(
            src_ref=xsend.at[to],
            dst_ref=xsums.at[me_dp],
            send_sem=xss,
            recv_sem=xsr,
            device_id={"dp": to},
            device_id_type=MESH,
        ).start()
    text_total = zbuf[0]
    for s in range(1, owners):
        text_total = text_total + zbuf[s]
    tsums[me_t] = text_total
    for k in spiral(tensors):
        to = peer(me_t, k, tensors)
        pltpu.make_async_remote_copy(
            src_ref=tsums.at[me_t],
            dst_ref=tsums.at[me_t],
            send_sem=tss,
            recv_sem=tsr,
            device_id={"tensor": to},
            device_id_type=MESH,
        ).start()
    for h in range(3, CHUNKS):
        send_chunk(h)
    xsums[me_dp] = xsend[me_dp]
    wait_for(tsums.at[pl.ds(0, tensors - 1)], tsr)
    wait_for(xsums.at[pl.ds(0, replicas - 1)], xsr)

    def scale_rows(q, carry):
        for i in range(UNROLL):
            p = q * UNROLL + i
            slot = kinv[p]
            safe = jnp.maximum(slot, 0)
            image = xsums[safe // 2, pl.ds(lax.rem(safe, 2), 1), :]
            total = jnp.where(slot >= 0, image, tsums[p // share, pl.ds(lax.rem(p, share), 1), :])
            scale = lax.rsqrt(total / D + 1e-05)
            scales[p] = jnp.transpose(jnp.broadcast_to(scale, (TILE, TILE)))
        return carry

    lax.fori_loop(0, positions // UNROLL, scale_rows, 0)

    stores = []
    for h in range(CHUNKS):
        wait_for(inc[h].at[pl.ds(0, CAP * (replicas - 1))], xr.at[h])

        here = pl.ds(base[h], SPANS[h])

        def finish(q, carry, h=h, here=here):
            for i in range(UNROLL):
                p = q * UNROLL + i
                slot = kinv[p]
                picked = inc[h][jnp.maximum(slot, 0)]
                chosen = jnp.where(slot >= 0, picked, text[p, here, :]).astype(jnp.float32)
                out[p, here, :] = (chosen * scales[p, here, :] * gain[...]).astype(jnp.bfloat16)
            return carry

        lax.fori_loop(0, positions // UNROLL, finish, 0)
        stores.append(
            pltpu.make_async_copy(out.at[:, here, :], out_hbm.at[:, here, :], osem.at[h])
        )
        stores[-1].start()

    wait_for(text.at[pl.ds(0, 2 * (owners - 1))], zs)
    wait_for(text.at[pl.ds(0, CAP * (replicas - 1))], xs)
    wait_for(ybuf.at[pl.ds(0, tensors - 1)], ys)
    wait_for(zbuf.at[pl.ds(0, owners - 1)], zss)
    wait_for(xsums.at[pl.ds(0, replicas - 1)], xss)
    wait_for(tsums.at[pl.ds(0, tensors - 1)], tss)
    for copy in stores:
        copy.wait()


def copy_kernel(source, target, held, in_sem, out_sem):
    parts = in_sem.shape[0]
    rows = held.shape[0] // parts
    loads, stores = [], []
    for i in range(parts):
        here = pl.ds(i * rows, rows)
        loads.append(pltpu.make_async_copy(source.at[here], held.at[here], in_sem.at[i]))
        stores.append(pltpu.make_async_copy(held.at[here], target.at[here], out_sem.at[i]))
        loads[-1].start()
    for load, store in zip(loads, stores):
        load.wait()
        store.start()
    for store in stores:
        store.wait()


def local(
    vit_out, ln_gain, ln_bias, proj_weight, proj_bias, text_embed, norm_gain, tile_dest, tile_place
):
    replicas, owners, tensors = (lax.axis_size(a) for a in ("dp", "seq", "tensor"))
    width = vit_out.shape[1]
    block = proj_weight.shape[2]
    positions = tile_place.shape[1]
    text = text_embed.reshape(positions, TILE, block)

    hbm = pl.BlockSpec(memory_space=pltpu.HBM)
    bf16, f32, i32 = jnp.bfloat16, jnp.float32, jnp.int32
    dma = pltpu.SemaphoreType.DMA

    def chunked(shape):
        return [pltpu.VMEM((*shape, span, block), bf16) for span in SPANS]

    out = pl.pallas_call(
        functools.partial(exchange_kernel, (replicas, owners, tensors, positions)),
        out_shape=jax.ShapeDtypeStruct(text.shape, bf16),
        in_specs=[hbm] * 9,
        out_specs=hbm,
        scratch_shapes=[
            pltpu.VMEM(text.shape, bf16),
            pltpu.VMEM((width // block, block), f32),
            pltpu.VMEM((width // block, block), f32),
            pltpu.VMEM(proj_bias.shape, f32),
            pltpu.VMEM((1, block), f32),
            pltpu.SMEM((tile_dest.shape[0],), i32),
            pltpu.SMEM(tile_place.shape, i32),
            pltpu.VMEM((1, width), f32),
            pltpu.VMEM((1, width), f32),
            pltpu.VMEM((width * owners, block), bf16),
            pltpu.VMEM((2, DEPTH * owners, block), f32),
            pltpu.VMEM((width, owners * block), bf16),
            pltpu.VMEM((2, 2 * max(sum(SPANS[h] for h in p) for p in PASSES), width), bf16),
            pltpu.VMEM((2 * SPANS[0], owners * block), f32),
            pltpu.VMEM((2, TILE, block), f32),
            pltpu.VMEM(text.shape, bf16),
            pltpu.VMEM(text.shape, f32),
            pltpu.VMEM((tensors, 8, TILE), f32),
            pltpu.VMEM((tensors, 8, TILE), f32),
            pltpu.VMEM((owners, 8, TILE), f32),
            pltpu.VMEM((2 * owners, TILE), f32),
            pltpu.VMEM((tensors, 8, TILE), f32),
            pltpu.VMEM((replicas, 8, TILE), f32),
            pltpu.VMEM((replicas, 8, TILE), f32),
            pltpu.SMEM((CAP * replicas,), i32),
            pltpu.SMEM((positions,), i32),
            pltpu.SMEM((replicas + 1,), i32),
        ]
        + chunked((owners, 2))
        + chunked((2 * owners,))
        + chunked((CAP * replicas,))
        + chunked((CAP * replicas,))
        + [pltpu.VMEM((2, span, width), bf16) for span in SPANS]
        + [dma, dma((CHUNKS,))] * 2
        + [dma] * 8
        + [dma, dma((CHUNKS,)), dma((width // DEPTH,)), dma((6,)), dma((CHUNKS,))],
        compiler_params=pltpu.CompilerParams(
            collective_id=0, has_side_effects=True, vmem_limit_bytes=LIMIT * 1024 * 1024
        ),
    )(
        vit_out.reshape(2, TILE, width),
        proj_weight.reshape(width * owners, block),
        ln_gain.reshape(-1, block),
        ln_bias.reshape(-1, block),
        proj_bias,
        text,
        norm_gain.reshape(1, block),
        tile_dest.reshape(-1),
        tile_place,
    )
    return pl.pallas_call(
        copy_kernel,
        out_shape=jax.ShapeDtypeStruct(text.shape, bf16),
        in_specs=[hbm],
        out_specs=hbm,
        scratch_shapes=[pltpu.VMEM(text.shape, bf16), dma((4,)), dma((4,))],
        compiler_params=pltpu.CompilerParams(vmem_limit_bytes=60 * 1024 * 1024),
    )(out).reshape(text_embed.shape)


def solution(mesh):
    placed = (
        P(("dp", "seq"), None),
        P(),
        P(),
        P(None, None, "tensor"),
        P(None, "tensor"),
        P("dp", ("seq", "tensor")),
        P(("seq", "tensor")),
        P(),
        P(),
    )
    return jax.shard_map(
        local, mesh=mesh, in_specs=placed, out_specs=P("dp", ("seq", "tensor")), check_vma=False
    )
```

```python
import functools

import jax
import jax.numpy as jnp
from jax import lax
from jax.experimental import pallas as pl
from jax.experimental.pallas import tpu as pltpu
from jax.sharding import PartitionSpec as P

D = 8192
TILE = 128
CAP = 2
SPANS = (16, 16, 32, 32, 32)
CHUNKS = len(SPANS)
DEPTH = 800
LIMIT = 56
PASSES = ((0,), (1,), (2,), (3, 4))
EARLY = 3
UNROLL = 4
MESH = pl.DeviceIdType.MESH


def spiral(n):
    order = [n // 2]
    for d in range(n // 2 - 1, 0, -1):
        order += [d, n - d]
    return order


def wait_for(ref, sem):
    pltpu.make_async_copy(ref, ref, sem).wait()


def lane_sums(squares):
    ones = jnp.ones((8, squares.shape[1]), jnp.bfloat16)
    dims = (((1,), (1,)), ((), ()))
    high = squares.astype(jnp.bfloat16)
    low = (squares - high.astype(jnp.float32)).astype(jnp.bfloat16)
    return lax.dot_general(
        ones, high, dims, preferred_element_type=jnp.float32
    ) + lax.dot_general(ones, low, dims, preferred_element_type=jnp.float32)


def exchange_kernel(
    sizes,
    vit_hbm,
    weight_hbm,
    ln_gain_hbm,
    ln_bias_hbm,
    bias_hbm,
    text_hbm,
    gain_hbm,
    dest_hbm,
    place_hbm,
    out_hbm,
    out,
    ln_gain,
    ln_bias,
    bias,
    gain,
    dest,
    place,
    lgain,
    lbias,
    wraw,
    wwide,
    wflat,
    xn,
    acc,
    squares,
    text,
    scales,
    part,
    ybuf,
    zbuf,
    isums,
    tsums,
    xsend,
    xsums,
    table,
    kinv,
    starts,
    *rest,
):
    replicas, owners, tensors, positions = sizes
    group_tiles = 2 * owners
    proj, tiles, slots, inc, vit = (rest[i * CHUNKS : (i + 1) * CHUNKS] for i in range(5))
    zs, zr, xs, xr, ys, yr, zss, zsr, xss, xsr, tss, tsr, tsem, vsem, wsem, psem, osem = rest[5 * CHUNKS :]
    width, block = vit_hbm.shape[2], gain.shape[1]
    steps = width // DEPTH
    me_dp, me_s, me_t = lax.axis_index("dp"), lax.axis_index("seq"), lax.axis_index("tensor")

    def peer(me, k, n):
        return lax.rem(me + k, n)

    small = []
    for i, (source, target) in enumerate(
        (
            (ln_gain_hbm, ln_gain),
            (ln_bias_hbm, ln_bias),
            (bias_hbm, bias),
            (gain_hbm, gain),
            (dest_hbm, dest),
            (place_hbm, place),
        )
    ):
        small.append(pltpu.make_async_copy(source, target, psem.at[i]))
        small[-1].start()
    base = [sum(SPANS[:h]) for h in range(CHUNKS)]
    load_vit = []
    for h in range(CHUNKS):
        here = pl.ds(base[h], SPANS[h])
        load_vit.append(
            pltpu.make_async_copy(vit_hbm.at[:, here, :], vit[h], vsem.at[h])
        )
    load_vit[0].start()
    load_weight = []
    for i in range(steps):
        here = pl.ds(i * DEPTH * owners, DEPTH * owners)
        load_weight.append(
            pltpu.make_async_copy(weight_hbm.at[here], wraw.at[here], wsem.at[i])
        )
    for copy in load_weight:
        copy.start()
    for copy in load_vit[1:]:
        copy.start()
    load_text = pltpu.make_async_copy(text_hbm, text, tsem)
    load_text.start()
    barrier = pltpu.get_barrier_semaphore()
    axes = (("dp", me_dp, replicas), ("seq", me_s, owners), ("tensor", me_t, tensors))
    for name, me, n in axes:
        for k in spiral(n):
            pl.semaphore_signal(
                barrier, inc=1, device_id={name: peer(me, k, n)}, device_id_type=MESH
            )

    def norm_chunk(h, side, first):
        load_vit[h].wait()

        def norm(g, carry):
            for i in range(2):
                rows = pl.ds(pl.multiple_of(16 * g, 16), 16)
                values = vit[h][i, rows, :].astype(jnp.float32)
                center = values - jnp.mean(values, axis=-1, keepdims=True)
                spread = jnp.mean(center * center, axis=-1, keepdims=True)
                normed = center * lax.rsqrt(spread + 1e-06) * lgain[...] + lbias[...]
                to = pl.ds(pl.multiple_of(first + i * SPANS[h] + 16 * g, 16), 16)
                xn[side, to, :] = normed.astype(jnp.bfloat16)
            return carry

        lax.fori_loop(0, SPANS[h] // 16, norm, 0)

    def keep(h, s, hidden):
        rounded = (hidden + bias[s : s + 1, :]).astype(jnp.bfloat16)
        proj[h][s] = rounded.reshape(2, SPANS[h], block)
        values = rounded.astype(jnp.float32)
        return (values * values).reshape(2, SPANS[h], block)


    def send_owners(h):
        for k in spiral(owners):
            to = peer(me_s, k, owners)
            pltpu.make_async_remote_copy(
                src_ref=proj[h].at[to],
                dst_ref=tiles[h].at[pl.ds(2 * me_s, 2)],
                send_sem=zs,
                recv_sem=zr.at[h],
                device_id={"seq": to},
                device_id_type=MESH,
            ).start()
        tiles[h][pl.ds(2 * me_s, 2)] = proj[h][me_s]

    small[0].wait()
    small[1].wait()
    for i in range(width // block):
        here = slice(i * block, (i + 1) * block)
        lgain[:, here] = ln_gain[i : i + 1, :]
        lbias[:, here] = ln_bias[i : i + 1, :]

    norm_chunk(0, 0, 0)
    first_rows = 2 * SPANS[0]

    def widen(i):
        load_weight[i].wait()
        here = pl.ds(i * DEPTH * owners, DEPTH * owners)
        wwide[i % 2] = wraw[here, :].astype(jnp.float32)

    widen(0)
    for i in range(steps):
        if i + 1 < steps:
            widen(i + 1)
        parts = [
            wwide[i % 2, pl.ds(s, DEPTH, stride=owners), :].astype(jnp.bfloat16)
            for s in range(owners)
        ]
        flat = jnp.concatenate(parts, axis=1)
        wflat[i * DEPTH : (i + 1) * DEPTH, :] = flat
        step = jnp.dot(
            xn[0, :first_rows, i * DEPTH : (i + 1) * DEPTH],
            flat,
            preferred_element_type=jnp.float32,
        )
        if i == 0:
            acc[...] = step
        else:
            acc[...] += step
    small[2].wait()
    total = jnp.zeros((2, SPANS[0], block), jnp.float32)
    for s in range(owners):
        total = total + keep(0, s, acc[:, s * block : (s + 1) * block])
    squares[:, 0 : SPANS[0], :] = total
    pl.semaphore_wait(barrier, replicas + owners + tensors - 3)
    send_owners(0)

    half = owners // 2

    def project(n_pass):
        rows = 0
        for h in PASSES[n_pass]:
            norm_chunk(h, n_pass % 2, rows)
            rows += 2 * SPANS[h]
        totals = [jnp.zeros((2, SPANS[h], block), jnp.float32) for h in PASSES[n_pass]]
        for n in range(2):
            hidden = jnp.dot(
                xn[n_pass % 2, :rows, :],
                wflat[:, n * half * block : (n + 1) * half * block],
                preferred_element_type=jnp.float32,
            )
            first = 0
            for i, h in enumerate(PASSES[n_pass]):
                mine = hidden[first : first + 2 * SPANS[h]]
                first += 2 * SPANS[h]
                for s in range(half):
                    columns = mine[:, s * block : (s + 1) * block]
                    totals[i] = totals[i] + keep(h, n * half + s, columns)
        for i, h in enumerate(PASSES[n_pass]):
            squares[:, base[h] : base[h] + SPANS[h], :] = totals[i]
            send_owners(h)

    for copy in small[3:]:
        copy.wait()
    for r in range(replicas):
        first = jnp.int32(group_tiles - 1)
        last = jnp.int32(0)
        for j in range(group_tiles):
            hit = dest[me_dp * group_tiles + j] == r
            last = jnp.where(hit, j, last)
            hit_back = dest[me_dp * group_tiles + group_tiles - 1 - j] == r
            first = jnp.where(hit_back, group_tiles - 1 - j, first)
        table[2 * r] = first
        table[2 * r + 1] = last

    for n_pass in range(1, EARLY):
        project(n_pass)


    def send_chunk(h):
        wait_for(tiles[h].at[pl.ds(0, 2 * (owners - 1))], zr.at[h])
        for k in spiral(replicas) + [0]:
            r = peer(me_dp, k, replicas)
            for c in range(CAP):
                slots[h][2 * r + c] = tiles[h][table[2 * r + c]]
        for k in spiral(replicas):
            to = peer(me_dp, k, replicas)
            pltpu.make_async_remote_copy(
                src_ref=slots[h].at[pl.ds(2 * to, 2)],
                dst_ref=inc[h].at[pl.ds(2 * me_dp, 2)],
                send_sem=xs,
                recv_sem=xr.at[h],
                device_id={"dp": to},
                device_id_type=MESH,
            ).start()
        inc[h][pl.ds(2 * me_dp, 2)] = slots[h][pl.ds(2 * me_dp, 2)]

    load_text.wait()
    sub = lax.broadcasted_iota(jnp.int32, (8, TILE), 0)
    share = positions // tensors

    def sum_text(t, carry):
        values = text[pl.ds(share * t, share)].astype(jnp.float32).reshape(share * TILE, TILE)
        sums = lane_sums(values * values)
        total = jnp.zeros((8, TILE), jnp.float32)
        for i in range(share):
            total = jnp.where(sub == i, sums[:, i * TILE : (i + 1) * TILE], total)
        part[t] = total
        return carry

    lax.fori_loop(0, tensors, sum_text, 0)
    send_chunk(0)
    for n_pass in range(EARLY, len(PASSES)):
        project(n_pass)
    sums = lane_sums(squares[...].reshape(2 * TILE, TILE))
    for t in range(tensors):
        for i in range(2):
            part[t, share + i : share + i + 1, :] = sums[:1, i * TILE : (i + 1) * TILE]
    for k in spiral(tensors):
        to = peer(me_t, k, tensors)
        pltpu.make_async_remote_copy(
            src_ref=part.at[to],
            dst_ref=ybuf.at[me_t],
            send_sem=ys,
            recv_sem=yr,
            device_id={"tensor": to},
            device_id_type=MESH,
        ).start()

    send_chunk(1)

    def count(g, total):
        starts[g] = total
        for j in range(group_tiles):
            total = total + jnp.where(dest[g * group_tiles + j] == me_dp, 1, 0)
        return total

    starts[replicas] = lax.fori_loop(0, replicas, count, jnp.int32(0))

    def invert(p, carry):
        order = jnp.int32(0)
        for k in range(positions):
            order = jnp.where(place[me_dp, k] == p, k, order)
        slot = jnp.int32(-1)
        for g in range(replicas):
            here = (order >= starts[g]) & (order < starts[g + 1])
            slot = jnp.where(here, 2 * g + order - starts[g], slot)
        kinv[p] = slot
        return carry

    lax.fori_loop(0, positions, invert, 0)

    wait_for(ybuf.at[pl.ds(0, tensors - 1)], yr)
    ybuf[me_t] = part[me_t]
    total = ybuf[0]
    for t in range(1, tensors):
        total = total + ybuf[t]
    zbuf[me_s] = total
    for k in spiral(owners):
        to = peer(me_s, k, owners)
        pltpu.make_async_remote_copy(
            src_ref=zbuf.at[me_s],
            dst_ref=zbuf.at[me_s],
            send_sem=zss,
            recv_sem=zsr,
            device_id={"seq": to},
            device_id_type=MESH,
        ).start()

    send_chunk(2)

    wait_for(zbuf.at[pl.ds(0, owners - 1)], zsr)
    for s in range(owners):
        isums[2 * s : 2 * s + 2, :] = zbuf[s, share : share + 2]
    for r in range(replicas):
        for c in range(CAP):
            xsend[r, c : c + 1, :] = isums[pl.ds(table[2 * r + c], 1), :]
    for k in spiral(replicas):
        to = peer(me_dp, k, replicas)
        pltpu.make_async_remote_copy(
            src_ref=xsend.at[to],
            dst_ref=xsums.at[me_dp],
            send_sem=xss,
            recv_sem=xsr,
            device_id={"dp": to},
            device_id_type=MESH,
        ).start()
    text_total = zbuf[0]
    for s in range(1, owners):
        text_total = text_total + zbuf[s]
    tsums[me_t] = text_total
    for k in spiral(tensors):
        to = peer(me_t, k, tensors)
        pltpu.make_async_remote_copy(
            src_ref=tsums.at[me_t],
            dst_ref=tsums.at[me_t],
            send_sem=tss,
            recv_sem=tsr,
            device_id={"tensor": to},
            device_id_type=MESH,
        ).start()
    for h in range(3, CHUNKS):
        send_chunk(h)
    xsums[me_dp] = xsend[me_dp]
    wait_for(tsums.at[pl.ds(0, tensors - 1)], tsr)
    wait_for(xsums.at[pl.ds(0, replicas - 1)], xsr)

    def scale_rows(q, carry):
        for i in range(UNROLL):
            p = q * UNROLL + i
            slot = kinv[p]
            safe = jnp.maximum(slot, 0)
            image = xsums[safe // 2, pl.ds(lax.rem(safe, 2), 1), :]
            total = jnp.where(slot >= 0, image, tsums[p // share, pl.ds(lax.rem(p, share), 1), :])
            scale = lax.rsqrt(total / D + 1e-05)
            scales[p] = jnp.transpose(jnp.broadcast_to(scale, (TILE, TILE)))
        return carry

    lax.fori_loop(0, positions // UNROLL, scale_rows, 0)

    stores = []
    for h in range(CHUNKS):
        wait_for(inc[h].at[pl.ds(0, CAP * (replicas - 1))], xr.at[h])

        here = pl.ds(base[h], SPANS[h])

        def finish(q, carry, h=h, here=here):
            for i in range(UNROLL):
                p = q * UNROLL + i
                slot = kinv[p]
                picked = inc[h][jnp.maximum(slot, 0)]
                chosen = jnp.where(slot >= 0, picked, text[p, here, :]).astype(jnp.float32)
                out[p, here, :] = (chosen * scales[p, here, :] * gain[...]).astype(jnp.bfloat16)
            return carry

        lax.fori_loop(0, positions // UNROLL, finish, 0)
        stores.append(
            pltpu.make_async_copy(out.at[:, here, :], out_hbm.at[:, here, :], osem.at[h])
        )
        stores[-1].start()

    wait_for(text.at[pl.ds(0, 2 * (owners - 1))], zs)
    wait_for(text.at[pl.ds(0, CAP * (replicas - 1))], xs)
    wait_for(ybuf.at[pl.ds(0, tensors - 1)], ys)
    wait_for(zbuf.at[pl.ds(0, owners - 1)], zss)
    wait_for(xsums.at[pl.ds(0, replicas - 1)], xss)
    wait_for(tsums.at[pl.ds(0, tensors - 1)], tss)
    for copy in stores:
        copy.wait()


def copy_kernel(source, target, held, in_sem, out_sem):
    parts = in_sem.shape[0]
    rows = held.shape[0] // parts
    loads, stores = [], []
    for i in range(parts):
        here = pl.ds(i * rows, rows)
        loads.append(pltpu.make_async_copy(source.at[here], held.at[here], in_sem.at[i]))
        stores.append(pltpu.make_async_copy(held.at[here], target.at[here], out_sem.at[i]))
        loads[-1].start()
    for load, store in zip(loads, stores):
        load.wait()
        store.start()
    for store in stores:
        store.wait()


def local(
    vit_out, ln_gain, ln_bias, proj_weight, proj_bias, text_embed, norm_gain, tile_dest, tile_place
):
    replicas, owners, tensors = (lax.axis_size(a) for a in ("dp", "seq", "tensor"))
    width = vit_out.shape[1]
    block = proj_weight.shape[2]
    positions = tile_place.shape[1]
    text = text_embed.reshape(positions, TILE, block)

    hbm = pl.BlockSpec(memory_space=pltpu.HBM)
    bf16, f32, i32 = jnp.bfloat16, jnp.float32, jnp.int32
    dma = pltpu.SemaphoreType.DMA

    def chunked(shape):
        return [pltpu.VMEM((*shape, span, block), bf16) for span in SPANS]

    out = pl.pallas_call(
        functools.partial(exchange_kernel, (replicas, owners, tensors, positions)),
        out_shape=jax.ShapeDtypeStruct(text.shape, bf16),
        in_specs=[hbm] * 9,
        out_specs=hbm,
        scratch_shapes=[
            pltpu.VMEM(text.shape, bf16),
            pltpu.VMEM((width // block, block), f32),
            pltpu.VMEM((width // block, block), f32),
            pltpu.VMEM(proj_bias.shape, f32),
            pltpu.VMEM((1, block), f32),
            pltpu.SMEM((tile_dest.shape[0],), i32),
            pltpu.SMEM(tile_place.shape, i32),
            pltpu.VMEM((1, width), f32),
            pltpu.VMEM((1, width), f32),
            pltpu.VMEM((width * owners, block), bf16),
            pltpu.VMEM((2, DEPTH * owners, block), f32),
            pltpu.VMEM((width, owners * block), bf16),
            pltpu.VMEM((2, 2 * max(sum(SPANS[h] for h in p) for p in PASSES), width), bf16),
            pltpu.VMEM((2 * SPANS[0], owners * block), f32),
            pltpu.VMEM((2, TILE, block), f32),
            pltpu.VMEM(text.shape, bf16),
            pltpu.VMEM(text.shape, f32),
            pltpu.VMEM((tensors, 8, TILE), f32),
            pltpu.VMEM((tensors, 8, TILE), f32),
            pltpu.VMEM((owners, 8, TILE), f32),
            pltpu.VMEM((2 * owners, TILE), f32),
            pltpu.VMEM((tensors, 8, TILE), f32),
            pltpu.VMEM((replicas, 8, TILE), f32),
            pltpu.VMEM((replicas, 8, TILE), f32),
            pltpu.SMEM((CAP * replicas,), i32),
            pltpu.SMEM((positions,), i32),
            pltpu.SMEM((replicas + 1,), i32),
        ]
        + chunked((owners, 2))
        + chunked((2 * owners,))
        + chunked((CAP * replicas,))
        + chunked((CAP * replicas,))
        + [pltpu.VMEM((2, span, width), bf16) for span in SPANS]
        + [dma, dma((CHUNKS,))] * 2
        + [dma] * 8
        + [dma, dma((CHUNKS,)), dma((width // DEPTH,)), dma((6,)), dma((CHUNKS,))],
        compiler_params=pltpu.CompilerParams(
            collective_id=0, has_side_effects=True, vmem_limit_bytes=LIMIT * 1024 * 1024
        ),
    )(
        vit_out.reshape(2, TILE, width),
        proj_weight.reshape(width * owners, block),
        ln_gain.reshape(-1, block),
        ln_bias.reshape(-1, block),
        proj_bias,
        text,
        norm_gain.reshape(1, block),
        tile_dest.reshape(-1),
        tile_place,
    )
    return pl.pallas_call(
        copy_kernel,
        out_shape=jax.ShapeDtypeStruct(text.shape, bf16),
        in_specs=[hbm],
        out_specs=hbm,
        scratch_shapes=[pltpu.VMEM(text.shape, bf16), dma((4,)), dma((4,))],
        compiler_params=pltpu.CompilerParams(vmem_limit_bytes=60 * 1024 * 1024),
    )(out).reshape(text_embed.shape)


def solution(mesh):
    placed = (
        P(("dp", "seq"), None),
        P(),
        P(),
        P(None, None, "tensor"),
        P(None, "tensor"),
        P("dp", ("seq", "tensor")),
        P(("seq", "tensor")),
        P(),
        P(),
    )
    return jax.shard_map(
        local, mesh=mesh, in_specs=placed, out_specs=P("dp", ("seq", "tensor")), check_vma=False
    )
```
